256 devices in a mesh: gx: 16 (over z_hi, x, core), gy: 16 (over y, z_lo).
Axes of the slice: x: 4, y: 4, z: 8 (z_hi: 2, z_lo: 4; z = z_hi * 4 + z_lo), core: 2. Of those that a mesh axis runs over, the one named last changes fastest.
Arguments:
- right_side: float32 [2, 256, 512, 128], P(None, 'gx', 'gy'), may hold values from -6 to 6
- wavenumber: float32 [256, 512, 128], P('gx', 'gy'), may hold values from 0.2 to 1
- pml_layer: int32 [256, 512, 128], P('gx', 'gy'), may hold values from 0 to 3
- aggregate: int32 [256, 512, 128], P('gx', 'gy'), may hold values from 0 to 15, as said below
- coarse_inverse: float32 [2, 4096, 4096], P(None, ('gx', 'gy')), may hold values from -0.0009765625 to 0.0009765625
Outputs:
- solution: float32 [2, 256, 512, 128], P(None, 'gx', 'gy')
- hessenberg: float32 [2, 5, 4], replicated
The draws below stay inside these ranges and needn't reach their ends.
Inputs may be any that keep to these rules, and one draw needn't show every extreme that they name: `aggregate`: along the third dimension the value never falls, and every value of 0 to 15 occurs in every column of cells.
All inputs are finite; a program needn't handle non-finite values.
Results may differ from the reference program's by a relative error of at most 0.00015.
Values sent between devices are 32-bit elements; how exact they have to be, the bound alone decides.
A program may use at most 64 MiB of HBM per device.

```python
import math
import jax
import jax.numpy as jnp
from jax import lax

CX = 16
CY = 32
CZ = 128
AGG_DEV = 16
ITERS = 4
NX = 256
NY = 512
NZ = 128
COARSE = 4096
N_GX = 16
N_GY = 16


def draw_aggregate(key, part):
    band = CZ // AGG_DEV
    offset = jax.random.randint(key, (NX, NY, 1), -(band // 2), band // 2 + 1, dtype=jnp.int32)
    depth = jnp.arange(NZ, dtype=jnp.int32)[None, None, :]
    return jnp.clip((depth + offset) // band, 0, AGG_DEV - 1).astype(jnp.int32)


def with_ends(entries, stream_key, low, high):
    shape = entries.shape
    spot = [jax.random.randint(jax.random.fold_in(stream_key, axis), (), 0, shape[axis]) for axis in range(len(shape))]
    entries = entries.at[tuple(spot)].set(low)
    longest = shape.index(max(shape))
    spot[longest] = (spot[longest] + 1) % shape[longest]
    return entries.at[tuple(spot)].set(high)


def shard_levels(stream_key, dims, cuts, low, high):
    level = 1.0
    for dim, parts in cuts:
        draws = jax.random.uniform(jax.random.fold_in(jax.random.fold_in(stream_key, 6), dim), (parts,), jnp.float32, low / len(cuts), high / len(cuts))
        level = level * jnp.repeat(jnp.exp(draws), dims[dim] // parts).reshape((-1,) + (1,) * (len(dims) - 1 - dim))
    return level


def scatter_about(rng, extent, width, bound, split=(), kind=jnp.bfloat16):
    result = jax.random.normal(rng, extent, jnp.float32) * width
    if len(split) > 0:
        result = shard_levels(rng, extent, split, -0.22, 0.18) * result
    return jnp.clip(result, min=-bound, max=bound).astype(kind)


def setup_inputs(seed: int = 0) -> dict:
    splits = jax.random.split(jax.random.key(seed), 6)
    right_side = scatter_about(splits[0], (2, NX, NY, NZ), 1.0, 6.0, ((1, 16), (2, 16)), jnp.float32)
    wavenumber = jnp.clip(jnp.exp(math.log(1.0) - 1.609438 * jax.random.uniform(splits[1], (NX, NY, NZ), jnp.float32) ** shard_levels(splits[1], (NX, NY, NZ), ((0, 16), (1, 16)), -0.2, 0.2)), 0.2, 1.0)
    pml_layer = with_ends(jax.random.randint(splits[2], (NX, NY, NZ), 0, 4), jax.random.fold_in(splits[2], 1), 0, 3).astype(jnp.int32)
    aggregate = draw_aggregate(jax.random.fold_in(splits[5], 71), 0)
    coarse_inverse = scatter_about(splits[4], (2, COARSE, COARSE), (2 * COARSE * CX * CY * (CZ // AGG_DEV)) ** -0.5, 0.0009765625, ((1, 256),), jnp.float32)
    return {"right_side": right_side, "wavenumber": wavenumber, "pml_layer": pml_layer, "aggregate": aggregate, "coarse_inverse": coarse_inverse}


damping = 0.8
pml_strength = 3.0
epsilon = 1e-06

def coefficients(wavenumber, layer_float):
    wave_sq = wavenumber * wavenumber
    depth = layer_float / 3.0
    absorb = wave_sq * (pml_strength * depth * depth)
    diag_re = 6.0 - wave_sq
    magnitude = diag_re * diag_re + absorb * absorb
    return (wave_sq, absorb, damping * diag_re / magnitude, damping * absorb / magnitude)

def operate(field, wave_sq, absorb):
    padded = jnp.pad(field, ((0, 0), (1, 1), (1, 1), (1, 1)))
    beside = padded[:, 2:, 1:-1, 1:-1] + padded[:, :-2, 1:-1, 1:-1] + padded[:, 1:-1, 2:, 1:-1] + padded[:, 1:-1, :-2, 1:-1] + padded[:, 1:-1, 1:-1, 2:] + padded[:, 1:-1, 1:-1, :-2]
    real_part = (6.0 - wave_sq) * field[0] - beside[0] + absorb * field[1]
    imag_part = (6.0 - wave_sq) * field[1] - beside[1] - absorb * field[0]
    return jnp.stack([real_part, imag_part])

def smooth(field, scale_re, scale_im):
    return jnp.stack([scale_re * field[0] - scale_im * field[1], scale_re * field[1] + scale_im * field[0]])

def complex_scale(scale_re, scale_im, field):
    return jnp.stack([scale_re * field[0] - scale_im * field[1], scale_re * field[1] + scale_im * field[0]])

def inner(left, right):
    return jnp.stack([jnp.sum(left[0] * right[0] + left[1] * right[1]), jnp.sum(left[0] * right[1] - left[1] * right[0])])

def least_squares(hessenberg, beta):
    real_h = hessenberg[0]
    imag_h = hessenberg[1]
    stacked = jnp.concatenate([jnp.concatenate([real_h, -imag_h], 1), jnp.concatenate([imag_h, real_h], 1)], 0)
    count = stacked.shape[1]
    target = jnp.zeros((stacked.shape[0],), jnp.float32).at[0].set(beta)
    ortho = []
    upper = {}
    for column in range(count):
        vector = stacked[:, column]
        for position in range(column):
            upper[position, column] = jnp.zeros((), jnp.float32)
        for repeat in range(2):
            for position in range(len(ortho)):
                weight = jnp.sum(ortho[position] * vector)
                vector = vector - weight * ortho[position]
                upper[position, column] = upper[position, column] + weight
        norm_value = jnp.sqrt(jnp.sum(vector * vector))
        upper[column, column] = norm_value
        ortho.append(vector / norm_value)
    project = [jnp.sum(basis_vec * target) for basis_vec in ortho]
    solved = [None] * count
    for column in reversed(range(count)):
        total = project[column]
        for later in range(column + 1, count):
            total = total - upper[column, later] * solved[later]
        solved[column] = total / upper[column, column]
    return solved

def precondition(vector, wave_sq, absorb, scale_re, scale_im, global_ids, coarse_inverse):
    highest = lax.Precision.HIGHEST
    first = smooth(vector, scale_re, scale_im)
    second = first + smooth(vector - operate(first, wave_sq, absorb), scale_re, scale_im)
    remainder = vector - operate(second, wave_sq, absorb)
    coarse_rhs = jax.ops.segment_sum(remainder.reshape(2, -1).T, global_ids, num_segments=COARSE).T
    coarse_re = jnp.dot(coarse_inverse[0], coarse_rhs[0], precision=highest) - jnp.dot(coarse_inverse[1], coarse_rhs[1], precision=highest)
    coarse_im = jnp.dot(coarse_inverse[0], coarse_rhs[1], precision=highest) + jnp.dot(coarse_inverse[1], coarse_rhs[0], precision=highest)
    spread = jnp.stack([coarse_re[global_ids], coarse_im[global_ids]]).reshape(remainder.shape)
    return second + spread

def reference(right_side, wavenumber, pml_layer, aggregate, coarse_inverse):
    wave_sq, absorb, scale_re, scale_im = coefficients(wavenumber, pml_layer.astype(jnp.float32))
    owner_x = jnp.arange(NX, dtype=jnp.int32) // (NX // N_GX)
    owner_y = jnp.arange(NY, dtype=jnp.int32) // (NY // N_GY)
    owner = (owner_x[:, None] * N_GY + owner_y[None, :]) * AGG_DEV
    global_ids = (owner[:, :, None] + aggregate).reshape(-1).astype(jnp.int32)
    beta = jnp.sqrt(jnp.sum(right_side * right_side) + epsilon)
    basis = [right_side / beta]
    directions = []
    columns_re = []
    columns_im = []
    for column in range(ITERS):
        direction = precondition(basis[column], wave_sq, absorb, scale_re, scale_im, global_ids, coarse_inverse)
        image = operate(direction, wave_sq, absorb)
        dots = jnp.stack([inner(vector, image) for vector in basis], 1)
        for position in range(len(basis)):
            image = image - complex_scale(dots[0, position], dots[1, position], basis[position])
        length = jnp.sqrt(jnp.sum(image * image) + epsilon)
        tail = jnp.zeros((ITERS - 1 - column,), jnp.float32)
        columns_re.append(jnp.concatenate([dots[0], length[None], tail]))
        columns_im.append(jnp.concatenate([dots[1], jnp.zeros((1,), jnp.float32), tail]))
        directions.append(direction)
        if column + 1 < ITERS:
            basis.append(image / length)
    hessenberg = jnp.stack([jnp.stack(columns_re, 1), jnp.stack(columns_im, 1)])
    solved = least_squares(hessenberg, beta)
    solution = jnp.zeros_like(right_side)
    for column in range(ITERS):
        solution = solution + complex_scale(solved[column], solved[ITERS + column], directions[column])
    return (solution, hessenberg)
```

```python
import functools

import jax
import jax.numpy as jnp
from jax import lax
from jax.experimental import pallas as pl
from jax.experimental.pallas import tpu as pltpu
from jax.sharding import Mesh
from jax.sharding import PartitionSpec as P

ITERS = 4
AXES = ("zh", "px", "co", "py", "zl")
GX = ("zh", "px", "co")
GY = ("py", "zl")
damping = 0.8
pml_strength = 3.0
epsilon = 1e-06

FRONT = 8
PITCH = 40
HALO = 3
NXD = 16
NYD = 32
ROWS = FRONT + (NXD + 2 * HALO) * PITCH
MESH = pl.DeviceIdType.MESH
DIRS = [(-1, -1), (-1, 0), (-1, 1), (0, -1), (0, 1), (1, -1), (1, 0), (1, 1)]
CORNERS = [(-1, -1), (-1, 1), (1, -1), (1, 1)]
F32 = jnp.float32


def row_of(e, t=0):
    return FRONT + e * PITCH + t * 8


def kernel(
    rhs, wave, layer, agg, cinv,
    sol, hess,
    wv, lf, ag, dg, ab, sr, si, idx,
    z, u, m, v, f, p, rem,
    dre, dim, g1, g2, cown, crecv,
    iy_s, iy_r, ic_s, ic_r, uy_s, uy_r, uc_s, uc_r,
    sem_s, sem_r,
):
    zh, px, co = lax.axis_index("zh"), lax.axis_index("px"), lax.axis_index("co")
    py, zl = lax.axis_index("py"), lax.axis_index("zl")
    gx = zh * 8 + px * 2 + co
    gy = py * 4 + zl
    s1 = (zh * 2 + co) * 4 + zl
    s2 = px * 4 + py

    def device(a, b):
        return (
            lax.div(a, 8), lax.rem(lax.div(a, 2), 4), lax.rem(a, 2), lax.div(b, 4), lax.rem(b, 4)
        )

    def beside_device(dx, dy):
        return device(lax.rem(gx + 16 + dx, 16), lax.rem(gy + 16 + dy, 16))

    def member1(k):
        s = lax.rem(s1 + k, 16)
        return (lax.div(s, 8), px, lax.rem(lax.div(s, 4), 2), py, lax.rem(s, 4))

    def member2(k):
        s = lax.rem(s2 + k, 16)
        return (zh, lax.div(s, 4), co, lax.rem(s, 4), zl)

    lane = lax.broadcasted_iota(jnp.int32, (8, 128), 1)
    sub = lax.broadcasted_iota(jnp.int32, (8, 128), 0)
    lane1 = lax.broadcasted_iota(jnp.int32, (1, 128), 1)
    zero = jnp.zeros((8, 128), F32)

    barrier = pltpu.get_barrier_semaphore()
    for dx, dy in DIRS:
        pl.semaphore_signal(barrier, inc=1, device_id=beside_device(dx, dy), device_id_type=MESH)

    def greet(k, carry):
        pl.semaphore_signal(barrier, inc=1, device_id=member1(k), device_id_type=MESH)
        pl.semaphore_signal(barrier, inc=1, device_id=member2(k), device_id_type=MESH)
        return carry

    lax.fori_loop(1, 16, greet, 0)

    def send(src, dst, kind, target):
        pltpu.make_async_remote_copy(
            src_ref=src,
            dst_ref=dst,
            send_sem=sem_s.at[kind],
            recv_sem=sem_r.at[kind],
            device_id=target,
            device_id_type=MESH,
        ).start()

    def take(like, sem):
        pltpu.make_async_copy(like, like, sem).wait()

    def coefficients(w, lay):
        wave_sq = w * w
        depth = lay / 3.0
        absorb = wave_sq * (pml_strength * depth * depth)
        diag = 6.0 - wave_sq
        magnitude = diag * diag + absorb * absorb
        return diag, absorb, damping * diag / magnitude, damping * absorb / magnitude

    def own_rows(x, carry):
        for t in range(4):
            here = pl.ds(pl.multiple_of(row_of(x + HALO, t), 8), 8)
            there = pl.ds(8 * t, 8)
            w = wave[x, there, :]
            lay = layer[x, there, :].astype(F32)
            which = agg[x, there, :]
            wv[here, :] = w
            lf[here, :] = lay
            ag[here, :] = which.astype(F32)
            idx[here, :] = which
            d, a, r, i = coefficients(w, lay)
            dg[here, :] = d
            ab[here, :] = a
            sr[here, :] = r
            si[here, :] = i
            z[0, 0, here, :] = rhs[0, x, there, :]
            z[0, 1, here, :] = rhs[1, x, there, :]
        return carry

    lax.fori_loop(0, NXD, own_rows, 0)

    def clear(k, carry):
        ag[pl.ds(pl.multiple_of(k * PITCH, 8), 8), :] = zero
        return carry

    lax.fori_loop(0, NXD + 2 * HALO + 1, clear, 0)

    def y_columns(ref, y):
        return ref[pl.ds(row_of(HALO) + y, NXD, stride=PITCH), :]

    def pack_y(buf, fields):
        at = 0
        for ref, width in fields:
            for s in range(width):
                buf[0, at] = y_columns(ref, s)
                buf[1, at] = y_columns(ref, NYD - width + s)
                at += 1

    def unpack_y(buf, fields):
        at = 0
        for ref, width in fields:
            for s in range(width):
                ref[pl.ds(row_of(HALO) + NYD + s, NXD, stride=PITCH), :] = buf[0, at]
                ref[pl.ds(row_of(HALO) - width + s, NXD, stride=PITCH), :] = buf[1, at]
                at += 1

    def send_x(fields, kind):
        for ref, width in fields:
            for s in range(width):
                low = pl.ds(row_of(HALO + s), NYD)
                high = pl.ds(row_of(HALO + NXD - width + s), NYD)
                past = pl.ds(row_of(HALO + NXD + s), NYD)
                ahead = pl.ds(row_of(HALO - width + s), NYD)
                send(ref.at[low], ref.at[past], kind, beside_device(-1, 0))
                send(ref.at[high], ref.at[ahead], kind, beside_device(1, 0))

    def send_y(out, into, kind):
        send(out.at[0], into.at[0], kind, beside_device(0, -1))
        send(out.at[1], into.at[1], kind, beside_device(0, 1))

    def edge_row(dx, dy, ox, oy):
        x = ox if dx < 0 else NXD - 1 - ox
        y = oy if dy < 0 else NYD - 1 - oy
        return row_of(HALO + x) + y

    def past_row(dx, dy, ox, oy):
        x = -1 - ox if dx < 0 else NXD + ox
        y = -1 - oy if dy < 0 else NYD + oy
        return row_of(HALO + x) + y

    def pack_corners(buf, cells):
        for k, (dx, dy) in enumerate(CORNERS):
            for at, (ref, ox, oy) in enumerate(cells):
                buf[k, pl.ds(at, 1), :] = ref[pl.ds(edge_row(dx, dy, ox, oy), 1), :]

    def send_corners(out, into, kind):
        for k, (dx, dy) in enumerate(CORNERS):
            send(out.at[k], into.at[3 - k], kind, beside_device(dx, dy))

    def unpack_corners(buf, cells):
        for k, (dx, dy) in enumerate(CORNERS):
            for at, (ref, ox, oy) in enumerate(cells):
                ref[pl.ds(past_row(dx, dy, ox, oy), 1), :] = buf[k, pl.ds(at, 1), :]

    first_fields = [(z.at[0, 0], 2), (z.at[0, 1], 2), (wv, 2), (lf, 2), (ag, 3)]
    first_cells = [(ref, 0, 0) for ref, _ in first_fields] + [(ag, 1, 0), (ag, 0, 1)]
    pack_y(iy_s, first_fields)
    pack_corners(ic_s, first_cells)

    pl.semaphore_wait(barrier, len(DIRS) + 30)

    send_x(first_fields, 0)
    send_y(iy_s, iy_r, 1)
    send_corners(ic_s, ic_r, 2)

    lane16 = lax.broadcasted_iota(jnp.int32, (16, 128), 1)
    low16 = lane16 < 64

    def arrange(a, carry):
        at_a = lax.rem(lax.div(a, 2), 4) * 16 + lax.div(a, 8) * 2 + lax.rem(a, 2)
        for half in range(2):
            cols = pl.ds(pl.multiple_of(a * 256 + half * 128, 128), 128)
            c_re, c_im = cinv[0, :, cols], cinv[1, :, cols]
            r_re, r_im = pltpu.roll(c_re, 64, axis=1), pltpu.roll(c_im, 64, axis=1)
            at = at_a + (2 * half) * 4
            dre[at] = jnp.where(low16, c_re, -r_im)
            dim[at] = jnp.where(low16, c_im, r_re)
            dre[at + 4] = jnp.where(low16, r_re, -c_im)
            dim[at + 4] = jnp.where(low16, r_im, c_re)
        return carry

    lax.fori_loop(0, 16, arrange, 0)

    take(u.at[0, 0, pl.ds(0, 22 * NYD)], sem_r.at[0])
    take(iy_r, sem_r.at[1])
    take(ic_r, sem_r.at[2])
    unpack_y(iy_r, first_fields)
    unpack_corners(ic_r, first_cells)

    def x_inside(e):
        below = jnp.where(gx > 0, 1, 0)
        above = jnp.where(gx < 15, 1, 0)
        return jnp.where(e < HALO, below, jnp.where(e >= HALO + NXD, above, 1))

    y_up = jnp.where(gy < 15, 1, 0)
    y_down = jnp.where(gy > 0, 1, 0)

    def halo_tile(e, t, with_coefficients):
        here = pl.ds(pl.multiple_of(row_of(e, t), 8), 8)
        if t < 4:
            inside = jnp.full((8, 128), x_inside(e), jnp.int32) > 0
        else:
            inside = jnp.where(sub < 4, x_inside(e) * y_up, x_inside(e + 1) * y_down) > 0
        idx[here, :] = jnp.where(inside, ag[here, :].astype(jnp.int32), 32)
        if with_coefficients:
            d, a, r, i = coefficients(wv[here, :], lf[here, :])
            dg[here, :] = d
            ab[here, :] = a
            sr[here, :] = jnp.where(inside, r, 0.0)
            si[here, :] = jnp.where(inside, i, 0.0)

    def y_halos(e, carry):
        halo_tile(e, 4, True)
        return carry

    halo_tile(-1, 4, False)
    lax.fori_loop(0, 21, y_halos, 0)
    halo_tile(21, 4, False)
    for low_e in (0, 19):

        def x_halos(k, carry):
            for t in range(4):
                halo_tile(low_e + k, t, True)
            return carry

        if low_e == 0:
            for t in range(4):
                halo_tile(0, t, False)
            lax.fori_loop(1, 3, x_halos, 0)
        else:
            lax.fori_loop(0, 2, x_halos, 0)
            for t in range(4):
                halo_tile(21, t, False)

    def neighbours(ref, c, base):
        centre = ref[c, pl.ds(base, 8), :]
        total = (
            ref[c, pl.ds(base + 1, 8), :]
            + ref[c, pl.ds(base - 1, 8), :]
            + ref[c, pl.ds(base + PITCH, 8), :]
            + ref[c, pl.ds(base - PITCH, 8), :]
        )
        up = jnp.where(lane == 127, 0.0, pltpu.roll(centre, 127, axis=1))
        down = jnp.where(lane == 0, 0.0, pltpu.roll(centre, 1, axis=1))
        return centre, total + up + down

    def operate(ref, base):
        c0, b0 = neighbours(ref, 0, base)
        c1, b1 = neighbours(ref, 1, base)
        here = pl.ds(base, 8)
        d, a = dg[here, :], ab[here, :]
        return c0, c1, d * c0 - b0 + a * c1, d * c1 - b1 - a * c0

    def over_tiles(width, body):
        low = HALO - width
        body(row_of(low - 1, 4))

        def rows(e, carry):
            for t in range(5):
                body(pl.multiple_of(row_of(e, t), 8))
            return carry

        lax.fori_loop(low, HALO + NXD + width, rows, 0)

    def smooth_all(j):
        zj, mj, uj = z.at[j], m.at[j], u.at[j]

        def make_first(base):
            here = pl.ds(base, 8)
            r, i = sr[here, :], si[here, :]
            a, b = zj[0, here, :], zj[1, here, :]
            f[0, here, :] = r * a - i * b
            f[1, here, :] = r * b + i * a

        over_tiles(2, make_first)

        def make_second(base):
            here = pl.ds(base, 8)
            f0, f1, w0, w1 = operate(f, base)
            r, i = sr[here, :], si[here, :]
            a, b = zj[0, here, :] - w0, zj[1, here, :] - w1
            mj[0, here, :] = f0 + (r * a - i * b)
            mj[1, here, :] = f1 + (r * b + i * a)

        over_tiles(1, make_second)

        def make_rest(x, carry):
            for t in range(4):
                base = pl.multiple_of(row_of(x + HALO, t), 8)
                here = pl.ds(base, 8)
                _, _, w0, w1 = operate(mj, base)
                uj[0, here, :] = w0
                uj[1, here, :] = w1
                rem[0, x, pl.ds(8 * t, 8), :] = zj[0, here, :] - w0
                rem[1, x, pl.ds(8 * t, 8), :] = zj[1, here, :] - w1
            return carry

        lax.fori_loop(0, NXD, make_rest, 0)

    def restrict():
        def rows(x, sums):
            sums = list(sums)
            for t in range(4):
                which = idx[pl.ds(pl.multiple_of(row_of(x + HALO, t), 8), 8), :]
                a, b = rem[0, x, pl.ds(8 * t, 8), :], rem[1, x, pl.ds(8 * t, 8), :]
                for g in range(16):
                    mask = which == g
                    sums[g] = sums[g] + jnp.where(mask, a, 0.0)
                    sums[16 + g] = sums[16 + g] + jnp.where(mask, b, 0.0)
            return tuple(sums)

        sums = lax.fori_loop(0, NXD, rows, (zero,) * 32)
        out = zero
        for k in range(32):
            place = (k // 16) * 64 + k % 16
            out = out + jnp.where(
                lane == zl * 16 + place, jnp.sum(sums[k], axis=1, keepdims=True), 0.0
            )
        return jnp.sum(out, axis=0, keepdims=True)

    def products(j):
        def rows(x, sums):
            sums = list(sums)
            for t in range(4):
                here = pl.ds(pl.multiple_of(row_of(x + HALO, t), 8), 8)
                a, b = z[j, 0, here, :], z[j, 1, here, :]
                sums[0] = sums[0] + (a * a + b * b)
                for i in range(j):
                    c, d = v[i, 0, here, :], v[i, 1, here, :]
                    sums[1 + 2 * i] = sums[1 + 2 * i] + (c * a + d * b)
                    sums[2 + 2 * i] = sums[2 + 2 * i] + (c * b - d * a)
            return tuple(sums)

        sums = lax.fori_loop(0, NXD, rows, (zero,) * (1 + 2 * j))
        out = zero
        for k, total in enumerate(sums):
            out = out + jnp.where(lane == k, jnp.sum(total, axis=1, keepdims=True), 0.0)
        return jnp.sum(out, axis=0, keepdims=True)

    S1, S2, CX, UX, UY, UC = 3, 8, 13, 17, 21, 25

    def start_gather(j, coarse, dots):
        mine = g1.at[j, pl.ds(2 * s1, 2)]
        g1[j, 2 * s1] = coarse if coarse is not None else jnp.zeros((1, 128), F32)
        g1[j, 2 * s1 + 1] = dots

        def step(k, carry):
            send(mine, mine, S1 + j, member1(k))
            return carry

        lax.fori_loop(1, 16, step, 0)

    def middle_gather(j):
        take(g1.at[j, pl.ds(0, 30)], sem_r.at[S1 + j])
        for q in range(4):
            g2[j, 5 * s2 + q] = (g1[j, 8 * q] + g1[j, 8 * q + 2]) + (
                g1[j, 8 * q + 4] + g1[j, 8 * q + 6]
            )
        total = g1[j, 1]
        for s in range(1, 16):
            total = total + g1[j, 2 * s + 1]
        g2[j, 5 * s2 + 4] = total
        mine = g2.at[j, pl.ds(5 * s2, 5)]

        def step(k, carry):
            send(mine, mine, S2 + j, member2(k))
            return carry

        lax.fori_loop(1, 16, step, 0)

    def end_gather(j):
        take(g2.at[j, pl.ds(0, 75)], sem_r.at[S2 + j])
        total = g2[j, 4]
        for s in range(1, 16):
            total = total + g2[j, 5 * s + 4]
        return [
            jnp.broadcast_to(
                jnp.sum(jnp.where(lane1 == k, total, 0.0), axis=1, keepdims=True), (8, 128)
            )
            for k in range(1 + 2 * j)
        ]

    sub16 = lax.broadcasted_iota(jnp.int32, (16, 128), 0)

    def coarse_solve(j):
        def step(k, sums):
            a, b = sums
            for q in range(4):
                row = g2[j, 5 * k + q]
                a = a + dre[4 * k + q] * row
                b = b + dim[4 * k + q] * row
            return a, b

        empty = jnp.zeros((16, 128), F32)
        a, b = lax.fori_loop(0, 16, step, (empty, empty))
        own = lane16 == sub16
        re = jnp.sum(
            jnp.where(own, jnp.sum(a, axis=1, keepdims=True), 0.0), axis=0, keepdims=True
        )
        im = jnp.sum(
            jnp.where(own, jnp.sum(b, axis=1, keepdims=True), 0.0), axis=0, keepdims=True
        )
        cown[j, 0] = re + pltpu.roll(jnp.broadcast_to(im, (8, 128)), 16, axis=1)[0:1]
        for k, (dx, dy) in enumerate(DIRS):
            send(cown.at[j], crecv.at[j, pl.ds(7 - k, 1)], CX + j, beside_device(dx, dy))
        return re, im

    def spread(table, here):
        which = idx[here, :]
        return (
            jnp.take_along_axis(table, which, axis=1, mode="promise_in_bounds"),
            jnp.take_along_axis(table, which + 16, axis=1, mode="promise_in_bounds"),
        )

    def prolong(j):
        take(crecv.at[j], sem_r.at[CX + j])

        def row(dx, dy):
            if (dx, dy) == (0, 0):
                return jnp.broadcast_to(cown[j, 0], (8, 128))
            return jnp.broadcast_to(crecv[j, DIRS.index((dx, dy))], (8, 128))

        def place(table, base):
            here = pl.ds(base, 8)
            a, b = spread(table, here)
            p[0, here, :] = a
            p[1, here, :] = b

        def side(e):
            return -1 if e < HALO else (1 if e >= HALO + NXD else 0)

        def halo_table(e):
            return jnp.where(sub < 4, row(side(e), 1), row(side(e + 1), -1))

        place(halo_table(-1), row_of(-1, 4))
        for e in [0, 1, 2, 18, 19, 20, 21]:
            table = row(side(e), 0)
            for t in range(4):
                place(table, row_of(e, t))
            place(halo_table(e), row_of(e, 4))
        table, edge = row(0, 0), halo_table(HALO)

        def rows(e, carry):
            for t in range(4):
                place(table, pl.multiple_of(row_of(e, t), 8))
            place(edge, pl.multiple_of(row_of(e, 4), 8))
            return carry

        lax.fori_loop(3, 18, rows, 0)

    def send_halo(j):
        fields = [(u.at[j, 0], 2), (u.at[j, 1], 2)]
        cells = [(u.at[j, 0], 0, 0), (u.at[j, 1], 0, 0)]
        pack_y(uy_s.at[j], fields)
        pack_corners(uc_s.at[j], cells)
        send_x(fields, UX + j)
        send_y(uy_s.at[j], uy_r.at[j], UY + j)
        send_corners(uc_s.at[j], uc_r.at[j], UC + j)

    def take_halo(j):
        fields = [(u.at[j, 0], 2), (u.at[j, 1], 2)]
        cells = [(u.at[j, 0], 0, 0), (u.at[j, 1], 0, 0)]
        take(z.at[4, 0, pl.ds(0, 8 * NYD)], sem_r.at[UX + j])
        take(uy_r.at[j], sem_r.at[UY + j])
        take(uc_r.at[j], sem_r.at[UC + j])
        unpack_y(uy_r.at[j], fields)
        unpack_corners(uc_r.at[j], cells)

    def over_own(body):
        def rows(x, carry):
            for t in range(4):
                body(pl.multiple_of(row_of(x + HALO, t), 8))
            return carry

        lax.fori_loop(0, NXD, rows, 0)

    columns = []
    lengths = []
    coarse = []

    def finish(j, dots):
        squared = dots[0]
        col = [(dots[1 + 2 * i], dots[2 + 2 * i]) for i in range(j)]
        for re, im in col:
            squared = squared - (re * re + im * im)
        if j > 0:
            squared = jnp.maximum(squared, 0.0)
            columns.append(col)
        lengths.append(jnp.sqrt(squared + epsilon))

    for j in range(ITERS):
        smooth_all(j)
        start_gather(j, restrict(), products(j))
        if j + 1 < ITERS:
            send_halo(j)
        middle_gather(j)
        if j + 1 < ITERS:
            take_halo(j)
        dots = end_gather(j)
        coarse.append(coarse_solve(j))
        finish(j, dots)
        inverse = 1.0 / lengths[j]
        col = columns[j - 1] if j else []

        def make_basis(base):
            here = pl.ds(base, 8)
            a, b = z[j, 0, here, :], z[j, 1, here, :]
            for i, (re, im) in enumerate(col):
                c, d = v[i, 0, here, :], v[i, 1, here, :]
                a = a - (re * c - im * d)
                b = b - (re * d + im * c)
            v[j, 0, here, :] = a * inverse
            v[j, 1, here, :] = b * inverse

        over_own(make_basis)

        def make_start(base):
            here = pl.ds(base, 8)
            a, b = u[j, 0, here, :], u[j, 1, here, :]
            for i, (re, im) in enumerate(col):
                c, d = z[i + 1, 0, here, :], z[i + 1, 1, here, :]
                a = a - (re * c - im * d)
                b = b - (re * d + im * c)
            z[j + 1, 0, here, :] = a
            z[j + 1, 1, here, :] = b

        if j + 1 < ITERS:
            over_tiles(2, make_start)
        else:
            over_own(make_start)
        prolong(j)

        def make_image(base):
            here = pl.ds(base, 8)
            _, _, w0, w1 = operate(p, base)
            z[j + 1, 0, here, :] = (z[j + 1, 0, here, :] + w0) * inverse
            z[j + 1, 1, here, :] = (z[j + 1, 1, here, :] + w1) * inverse

        if j + 1 < ITERS:
            over_tiles(2, make_image)
        else:
            over_own(make_image)

    start_gather(ITERS, None, products(ITERS))
    middle_gather(ITERS)
    finish(ITERS, end_gather(ITERS))

    def times(a, b):
        return (a[0] * b[0] - a[1] * b[1], a[0] * b[1] + a[1] * b[0])

    def conj_times(a, b):
        return (a[0] * b[0] + a[1] * b[1], a[0] * b[1] - a[1] * b[0])

    rotations, upper, diagonal = [], [], []
    target = [(lengths[0], zero)]
    for j in range(ITERS):
        col = list(columns[j])
        for k, (c, s) in enumerate(rotations):
            head, tail = col[k], col[k + 1]
            turned = conj_times(c, head)
            other = times(c, tail)
            col[k] = (turned[0] + s * tail[0], turned[1] + s * tail[1])
            col[k + 1] = (other[0] - s * head[0], other[1] - s * head[1])
        below = lengths[j + 1]
        a = col[j]
        size = jnp.sqrt(a[0] * a[0] + a[1] * a[1] + below * below)
        c, s = (a[0] / size, a[1] / size), below / size
        rotations.append((c, s))
        upper.append(col)
        diagonal.append(size)
        last = target[j]
        target[j] = conj_times(c, last)
        target.append((-s * last[0], -s * last[1]))
    solved = [None] * ITERS
    for j in reversed(range(ITERS)):
        re, im = target[j]
        for k in range(j + 1, ITERS):
            part = times(upper[k][j], solved[k])
            re, im = re - part[0], im - part[1]
        solved[j] = (re / diagonal[j], im / diagonal[j])

    weights = [None] * ITERS
    for j in reversed(range(ITERS)):
        inverse = 1.0 / lengths[j]
        weights[j] = (solved[j][0] * inverse, solved[j][1] * inverse)
        if j:
            for i, h in enumerate(columns[j - 1]):
                part = times(h, weights[j])
                solved[i] = (solved[i][0] - part[0], solved[i][1] - part[1])

    c_re, c_im = zero, zero
    for j in range(ITERS):
        wr, wi = weights[j]
        c_re = c_re + (wr * coarse[j][0] - wi * coarse[j][1])
        c_im = c_im + (wr * coarse[j][1] + wi * coarse[j][0])
    table = c_re + pltpu.roll(c_im, 16, axis=1)

    def write(x, carry):
        for t in range(4):
            here = pl.ds(pl.multiple_of(row_of(x + HALO, t), 8), 8)
            a, b = spread(table, here)
            for j in range(ITERS):
                wr, wi = weights[j]
                c, d = m[j, 0, here, :], m[j, 1, here, :]
                a = a + (wr * c - wi * d)
                b = b + (wr * d + wi * c)
            sol[0, x, pl.ds(8 * t, 8), :] = a
            sol[1, x, pl.ds(8 * t, 8), :] = b
        return carry

    lax.fori_loop(0, NXD, write, 0)

    h_re, h_im = zero, zero
    for j in range(ITERS):
        for i, (re, im) in enumerate(columns[j]):
            spot = (sub == i) & (lane == j)
            h_re = jnp.where(spot, re, h_re)
            h_im = jnp.where(spot, im, h_im)
        h_re = jnp.where((sub == j + 1) & (lane == j), lengths[j + 1], h_re)
    hess[0] = h_re
    hess[1] = h_im

    take(u.at[0, 0, pl.ds(0, 22 * NYD)], sem_s.at[0])
    take(iy_s, sem_s.at[1])
    take(ic_s, sem_s.at[2])
    for j in range(ITERS + 1):
        take(g1.at[j, pl.ds(0, 30)], sem_s.at[S1 + j])
        take(g2.at[j, pl.ds(0, 75)], sem_s.at[S2 + j])
    for j in range(ITERS):
        take(crecv.at[j], sem_s.at[CX + j])
        if j + 1 < ITERS:
            take(z.at[4, 0, pl.ds(0, 8 * NYD)], sem_s.at[UX + j])
            take(uy_s.at[j], sem_s.at[UY + j])
            take(uc_s.at[j], sem_s.at[UC + j])


def body(right_side, wavenumber, pml_layer, aggregate, coarse_inverse):
    field = pltpu.VMEM((2, ROWS, 128), F32)
    plane = pltpu.VMEM((ROWS, 128), F32)

    def fields(n):
        return pltpu.VMEM((n, 2, ROWS, 128), F32)

    vmem = pl.BlockSpec(memory_space=pltpu.VMEM)
    solution, hessenberg = pl.pallas_call(
        kernel,
        out_shape=(
            jax.ShapeDtypeStruct(right_side.shape, F32),
            jax.ShapeDtypeStruct((2, 8, 128), F32),
        ),
        in_specs=[vmem] * 5,
        out_specs=(vmem, vmem),
        scratch_shapes=[
            *[plane] * 7,
            pltpu.VMEM((ROWS, 128), jnp.int32),
            fields(5), fields(4), fields(4), fields(4),
            field, field,
            pltpu.VMEM((2, NXD, NYD, 128), F32),
            pltpu.VMEM((64, 16, 128), F32),
            pltpu.VMEM((64, 16, 128), F32),
            pltpu.VMEM((5, 32, 1, 128), F32),
            pltpu.VMEM((5, 80, 1, 128), F32),
            pltpu.VMEM((4, 1, 1, 128), F32),
            pltpu.VMEM((4, 8, 1, 128), F32),
            pltpu.VMEM((2, 11, 16, 128), F32),
            pltpu.VMEM((2, 11, 16, 128), F32),
            pltpu.VMEM((4, 8, 128), F32),
            pltpu.VMEM((4, 8, 128), F32),
            pltpu.VMEM((3, 2, 4, 16, 128), F32),
            pltpu.VMEM((3, 2, 4, 16, 128), F32),
            pltpu.VMEM((3, 4, 8, 128), F32),
            pltpu.VMEM((3, 4, 8, 128), F32),
            pltpu.SemaphoreType.DMA((28,)),
            pltpu.SemaphoreType.DMA((28,)),
        ],
        compiler_params=pltpu.CompilerParams(
            collective_id=0, has_side_effects=True, vmem_limit_bytes=60 * 1024 * 1024
        ),
    )(right_side, wavenumber, pml_layer, aggregate, coarse_inverse)
    return solution, hessenberg[:, : ITERS + 1, :ITERS]


def solution(mesh):
    finer = Mesh(mesh.devices.reshape(2, 4, 2, 4, 4), AXES)
    in_specs = (
        P(None, GX, GY, None),
        P(GX, GY, None),
        P(GX, GY, None),
        P(GX, GY, None),
        P(None, GX + GY, None),
    )
    out_specs = (P(None, GX, GY, None), P())
    return jax.shard_map(body, mesh=finer, in_specs=in_specs, out_specs=out_specs, check_vma=False)
```

```python
import functools

import jax
import jax.numpy as jnp
from jax import lax
from jax.experimental import pallas as pl
from jax.experimental.pallas import tpu as pltpu
from jax.sharding import Mesh
from jax.sharding import PartitionSpec as P

ITERS = 4
AXES = ("zh", "px", "co", "py", "zl")
GX = ("zh", "px", "co")
GY = ("py", "zl")
damping = 0.8
pml_strength = 3.0
epsilon = 1e-06

FRONT = 8
PITCH = 40
HALO = 3
NXD = 16
NYD = 32
ROWS = FRONT + (NXD + 2 * HALO) * PITCH
MESH = pl.DeviceIdType.MESH
DIRS = [(-1, -1), (-1, 0), (-1, 1), (0, -1), (0, 1), (1, -1), (1, 0), (1, 1)]
CORNERS = [(-1, -1), (-1, 1), (1, -1), (1, 1)]
F32 = jnp.float32


def over_rows(low, high, group, body):
    def trip(k, carry):
        for q in range(group):
            body(low + k * group + q)
        return carry

    lax.fori_loop(0, (high - low) // group, trip, 0)


def row_of(e, t=0):
    return FRONT + e * PITCH + t * 8


def kernel(
    rhs_in, wave_in, layer_in, agg_in, cinv_in,
    sol, hess,
    rhs, wave, layer, agg, cinv,
    wv, lf, ag, dg, ab, sr, si, idx,
    z, u, m, v, f, p, rem,
    dre, dim, g1, g2, cown, crecv,
    iy_s, iy_r, ic_s, ic_r, uy_s, uy_r, uc_s, uc_r,
    sem_s, sem_r, sem_in,
):
    zh, px, co = lax.axis_index("zh"), lax.axis_index("px"), lax.axis_index("co")
    py, zl = lax.axis_index("py"), lax.axis_index("zl")
    gx = zh * 8 + px * 2 + co
    gy = py * 4 + zl
    s1 = (zh * 2 + co) * 4 + zl
    s2 = px * 4 + py

    def device(a, b):
        return (
            lax.div(a, 8), lax.rem(lax.div(a, 2), 4), lax.rem(a, 2), lax.div(b, 4), lax.rem(b, 4)
        )

    def beside_device(dx, dy):
        return device(lax.rem(gx + 16 + dx, 16), lax.rem(gy + 16 + dy, 16))

    far = (2, 3, 1, 0)
    zhs = [zh, 1 - zh]
    cos = [co, 1 - co]
    zls = [zl] + [lax.rem(zl + k, 4) for k in range(1, 4)]
    pxs = [px] + [lax.rem(px + k, 4) for k in range(1, 4)]
    pys = [py] + [lax.rem(py + k, 4) for k in range(1, 4)]
    group1 = [
        (zhs[a], px, cos[b], py, zls[c])
        for a in (1, 0) for c in far for b in (1, 0) if (a, b, c) != (0, 0, 0)
    ]
    group2 = [
        (zh, pxs[a], co, pys[b], zl) for a in far for b in far if (a, b) != (0, 0)
    ]
    towards = {d: beside_device(*d) for d in DIRS}

    lane = lax.broadcasted_iota(jnp.int32, (8, 128), 1)
    sub = lax.broadcasted_iota(jnp.int32, (8, 128), 0)
    lane1 = lax.broadcasted_iota(jnp.int32, (1, 128), 1)
    zero = jnp.zeros((8, 128), F32)

    barrier = pltpu.get_barrier_semaphore()
    partners = group1 + group2 + list(towards.values())
    for target in partners:
        pl.semaphore_signal(barrier, inc=1, device_id=target, device_id_type=MESH)

    loads = [
        pltpu.make_async_copy(src, dst, sem_in.at[k])
        for k, (src, dst) in enumerate(
            [(wave_in, wave), (layer_in, layer), (agg_in, agg), (rhs_in, rhs), (cinv_in, cinv)]
        )
    ]
    for load in loads:
        load.start()

    def send(src, dst, kind, target):
        pltpu.make_async_remote_copy(
            src_ref=src,
            dst_ref=dst,
            send_sem=sem_s.at[kind],
            recv_sem=sem_r.at[kind],
            device_id=target,
            device_id_type=MESH,
        ).start()

    def take(like, sem):
        pltpu.make_async_copy(like, like, sem).wait()

    def coefficients(w, lay):
        wave_sq = w * w
        depth = lay / 3.0
        absorb = wave_sq * (pml_strength * depth * depth)
        diag = 6.0 - wave_sq
        magnitude = diag * diag + absorb * absorb
        return diag, absorb, damping * diag / magnitude, damping * absorb / magnitude

    for load in loads[:4]:
        load.wait()

    def own_rows(x):
        for t in range(4):
            here = pl.ds(pl.multiple_of(row_of(x + HALO, t), 8), 8)
            there = pl.ds(8 * t, 8)
            w = wave[x, there, :]
            lay = layer[x, there, :].astype(F32)
            which = agg[x, there, :]
            wv[here, :] = w
            lf[here, :] = lay
            ag[here, :] = which.astype(F32)
            idx[here, :] = which
            d, a, r, i = coefficients(w, lay)
            dg[here, :] = d
            ab[here, :] = a
            sr[here, :] = r
            si[here, :] = i
            z[0, 0, here, :] = rhs[0, x, there, :]
            z[0, 1, here, :] = rhs[1, x, there, :]

    over_rows(0, NXD, 2, own_rows)

    def clear(k, carry):
        ag[pl.ds(pl.multiple_of(k * PITCH, 8), 8), :] = zero
        return carry

    lax.fori_loop(0, NXD + 2 * HALO + 1, clear, 0)

    def y_columns(ref, y):
        return ref[pl.ds(row_of(HALO) + y, NXD, stride=PITCH), :]

    def pack_y(buf, fields):
        at = 0
        for ref, width in fields:
            for s in range(width):
                buf[0, at] = y_columns(ref, s)
                buf[1, at] = y_columns(ref, NYD - width + s)
                at += 1

    def unpack_y(buf, fields):
        at = 0
        for ref, width in fields:
            for s in range(width):
                ref[pl.ds(row_of(HALO) + NYD + s, NXD, stride=PITCH), :] = buf[0, at]
                ref[pl.ds(row_of(HALO) - width + s, NXD, stride=PITCH), :] = buf[1, at]
                at += 1

    def send_x(fields, kind):
        for ref, width in fields:
            for s in range(width):
                low = pl.ds(row_of(HALO + s), NYD)
                high = pl.ds(row_of(HALO + NXD - width + s), NYD)
                past = pl.ds(row_of(HALO + NXD + s), NYD)
                ahead = pl.ds(row_of(HALO - width + s), NYD)
                send(ref.at[low], ref.at[past], kind, towards[-1, 0])
                send(ref.at[high], ref.at[ahead], kind, towards[1, 0])

    def send_y(out, into, kind):
        send(out.at[0], into.at[0], kind, towards[0, -1])
        send(out.at[1], into.at[1], kind, towards[0, 1])

    def edge_row(dx, dy, ox, oy):
        x = ox if dx < 0 else NXD - 1 - ox
        y = oy if dy < 0 else NYD - 1 - oy
        return row_of(HALO + x) + y

    def past_row(dx, dy, ox, oy):
        x = -1 - ox if dx < 0 else NXD + ox
        y = -1 - oy if dy < 0 else NYD + oy
        return row_of(HALO + x) + y

    def pack_corners(buf, cells):
        for k, (dx, dy) in enumerate(CORNERS):
            for at, (ref, ox, oy) in enumerate(cells):
                buf[k, pl.ds(at, 1), :] = ref[pl.ds(edge_row(dx, dy, ox, oy), 1), :]

    def send_corners(out, into, kind):
        for k, (dx, dy) in enumerate(CORNERS):
            send(out.at[k], into.at[3 - k], kind, towards[dx, dy])

    def unpack_corners(buf, cells):
        for k, (dx, dy) in enumerate(CORNERS):
            for at, (ref, ox, oy) in enumerate(cells):
                ref[pl.ds(past_row(dx, dy, ox, oy), 1), :] = buf[k, pl.ds(at, 1), :]

    first_fields = [(z.at[0, 0], 2), (z.at[0, 1], 2), (wv, 2), (lf, 2), (ag, 3)]
    first_cells = [(ref, 0, 0) for ref, _ in first_fields] + [(ag, 1, 0), (ag, 0, 1)]
    pack_y(iy_s, first_fields)
    pack_corners(ic_s, first_cells)

    pl.semaphore_wait(barrier, len(partners))

    send_x(first_fields, 0)
    send_y(iy_s, iy_r, 1)
    send_corners(ic_s, ic_r, 2)

    lane16 = lax.broadcasted_iota(jnp.int32, (16, 128), 1)
    low16 = lane16 < 64

    def arrange(a, carry):
        at_a = lax.rem(lax.div(a, 2), 4) * 16 + lax.div(a, 8) * 2 + lax.rem(a, 2)
        for half in range(2):
            cols = pl.ds(pl.multiple_of(a * 256 + half * 128, 128), 128)
            c_re, c_im = cinv[0, :, cols], cinv[1, :, cols]
            r_re, r_im = pltpu.roll(c_re, 64, axis=1), pltpu.roll(c_im, 64, axis=1)
            at = at_a + (2 * half) * 4
            dre[at] = jnp.where(low16, c_re, -r_im)
            dim[at] = jnp.where(low16, c_im, r_re)
            dre[at + 4] = jnp.where(low16, r_re, -c_im)
            dim[at + 4] = jnp.where(low16, r_im, c_re)
        return carry

    loads[4].wait()
    lax.fori_loop(0, 16, arrange, 0)

    take(u.at[0, 0, pl.ds(0, 22 * NYD)], sem_r.at[0])
    take(iy_r, sem_r.at[1])
    take(ic_r, sem_r.at[2])
    unpack_y(iy_r, first_fields)
    unpack_corners(ic_r, first_cells)

    def x_inside(e):
        below = jnp.where(gx > 0, 1, 0)
        above = jnp.where(gx < 15, 1, 0)
        return jnp.where(e < HALO, below, jnp.where(e >= HALO + NXD, above, 1))

    y_up = jnp.where(gy < 15, 1, 0)
    y_down = jnp.where(gy > 0, 1, 0)

    def halo_tile(e, t, with_coefficients):
        here = pl.ds(pl.multiple_of(row_of(e, t), 8), 8)
        if t < 4:
            inside = jnp.full((8, 128), x_inside(e), jnp.int32) > 0
        else:
            inside = jnp.where(sub < 4, x_inside(e) * y_up, x_inside(e + 1) * y_down) > 0
        idx[here, :] = jnp.where(inside, ag[here, :].astype(jnp.int32), 32)
        if with_coefficients:
            d, a, r, i = coefficients(wv[here, :], lf[here, :])
            dg[here, :] = d
            ab[here, :] = a
            sr[here, :] = jnp.where(inside, r, 0.0)
            si[here, :] = jnp.where(inside, i, 0.0)

    def y_halos(e, carry):
        halo_tile(e, 4, True)
        return carry

    halo_tile(-1, 4, False)
    lax.fori_loop(0, 21, y_halos, 0)
    halo_tile(21, 4, False)
    for low_e in (0, 19):

        def x_halos(k, carry):
            for t in range(4):
                halo_tile(low_e + k, t, True)
            return carry

        if low_e == 0:
            for t in range(4):
                halo_tile(0, t, False)
            lax.fori_loop(1, 3, x_halos, 0)
        else:
            lax.fori_loop(0, 2, x_halos, 0)
            for t in range(4):
                halo_tile(21, t, False)

    def neighbours(ref, c, base):
        centre = ref[c, pl.ds(base, 8), :]
        total = (
            ref[c, pl.ds(base + 1, 8), :]
            + ref[c, pl.ds(base - 1, 8), :]
            + ref[c, pl.ds(base + PITCH, 8), :]
            + ref[c, pl.ds(base - PITCH, 8), :]
        )
        up = jnp.where(lane == 127, 0.0, pltpu.roll(centre, 127, axis=1))
        down = jnp.where(lane == 0, 0.0, pltpu.roll(centre, 1, axis=1))
        return centre, total + up + down

    def operate(ref, base):
        c0, b0 = neighbours(ref, 0, base)
        c1, b1 = neighbours(ref, 1, base)
        here = pl.ds(base, 8)
        d, a = dg[here, :], ab[here, :]
        return c0, c1, d * c0 - b0 + a * c1, d * c1 - b1 - a * c0

    def over_tiles(width, body, group):
        low = HALO - width
        body(row_of(low - 1, 4))

        def row(e):
            for t in range(5):
                body(pl.multiple_of(row_of(e, t), 8))

        over_rows(low, HALO + NXD + width, group, row)

    def put_first(here, a, b):
        r, i = sr[here, :], si[here, :]
        f[0, here, :] = r * a - i * b
        f[1, here, :] = r * b + i * a

    def smooth_all(j):
        zj, mj, uj = z.at[j], m.at[j], u.at[j]

        def make_first(base):
            here = pl.ds(base, 8)
            put_first(here, zj[0, here, :], zj[1, here, :])

        if j == 0:
            over_tiles(2, make_first, 4)

        def make_second(base):
            here = pl.ds(base, 8)
            f0, f1, w0, w1 = operate(f, base)
            r, i = sr[here, :], si[here, :]
            a, b = zj[0, here, :] - w0, zj[1, here, :] - w1
            mj[0, here, :] = f0 + (r * a - i * b)
            mj[1, here, :] = f1 + (r * b + i * a)

        over_tiles(1, make_second, 3)

        def make_rest(x):
            for t in range(4):
                base = pl.multiple_of(row_of(x + HALO, t), 8)
                here = pl.ds(base, 8)
                _, _, w0, w1 = operate(mj, base)
                uj[0, here, :] = w0
                uj[1, here, :] = w1
                rem[0, x, pl.ds(8 * t, 8), :] = zj[0, here, :] - w0
                rem[1, x, pl.ds(8 * t, 8), :] = zj[1, here, :] - w1

        over_rows(0, NXD, 4, make_rest)

    def restrict():
        def rows(x, sums):
            sums = list(sums)
            for t in range(4):
                which = idx[pl.ds(pl.multiple_of(row_of(x + HALO, t), 8), 8), :]
                a, b = rem[0, x, pl.ds(8 * t, 8), :], rem[1, x, pl.ds(8 * t, 8), :]
                for g in range(16):
                    mask = which == g
                    sums[g] = sums[g] + jnp.where(mask, a, 0.0)
                    sums[16 + g] = sums[16 + g] + jnp.where(mask, b, 0.0)
            return tuple(sums)

        sums = lax.fori_loop(0, NXD, rows, (zero,) * 32)
        out = zero
        for k in range(32):
            place = (k // 16) * 64 + k % 16
            out = out + jnp.where(
                lane == zl * 16 + place, jnp.sum(sums[k], axis=1, keepdims=True), 0.0
            )
        return jnp.sum(out, axis=0, keepdims=True)

    def products(j):
        def rows(x, sums):
            sums = list(sums)
            for t in range(4):
                here = pl.ds(pl.multiple_of(row_of(x + HALO, t), 8), 8)
                a, b = z[j, 0, here, :], z[j, 1, here, :]
                sums[0] = sums[0] + (a * a + b * b)
                for i in range(j):
                    c, d = v[i, 0, here, :], v[i, 1, here, :]
                    sums[1 + 2 * i] = sums[1 + 2 * i] + (c * a + d * b)
                    sums[2 + 2 * i] = sums[2 + 2 * i] + (c * b - d * a)
            return tuple(sums)

        sums = lax.fori_loop(0, NXD // 2, lambda k, c: rows(2 * k + 1, rows(2 * k, c)), (zero,) * (1 + 2 * j))
        out = zero
        for k, total in enumerate(sums):
            out = out + jnp.where(lane == k, jnp.sum(total, axis=1, keepdims=True), 0.0)
        return jnp.sum(out, axis=0, keepdims=True)

    S1, S2, CX, UX, UY, UC = 3, 8, 13, 17, 21, 25

    def start_gather(j, coarse, dots):
        mine = g1.at[j, pl.ds(2 * s1, 2)]
        g1[j, 2 * s1] = coarse if coarse is not None else jnp.zeros((1, 128), F32)
        g1[j, 2 * s1 + 1] = dots

        for target in group1:
            send(mine, mine, S1 + j, target)

    def middle_gather(j):
        take(g1.at[j, pl.ds(0, 30)], sem_r.at[S1 + j])
        for q in range(4):
            g2[j, 5 * s2 + q] = (g1[j, 8 * q] + g1[j, 8 * q + 2]) + (
                g1[j, 8 * q + 4] + g1[j, 8 * q + 6]
            )
        total = g1[j, 1]
        for s in range(1, 16):
            total = total + g1[j, 2 * s + 1]
        g2[j, 5 * s2 + 4] = total
        mine = g2.at[j, pl.ds(5 * s2, 5)]

        for target in group2:
            send(mine, mine, S2 + j, target)

    def end_gather(j):
        take(g2.at[j, pl.ds(0, 75)], sem_r.at[S2 + j])
        total = g2[j, 4]
        for s in range(1, 16):
            total = total + g2[j, 5 * s + 4]
        return [
            jnp.broadcast_to(
                jnp.sum(jnp.where(lane1 == k, total, 0.0), axis=1, keepdims=True), (8, 128)
            )
            for k in range(1 + 2 * j)
        ]

    sub16 = lax.broadcasted_iota(jnp.int32, (16, 128), 0)

    def coarse_solve(j):
        def step(k, sums):
            sums = list(sums)
            for o in range(4):
                for q in range(4):
                    row = g2[j, 20 * k + 5 * o + q]
                    at = 16 * k + 4 * o + q
                    sums[q % 2] = sums[q % 2] + dre[at] * row
                    sums[2 + q % 2] = sums[2 + q % 2] + dim[at] * row
            return tuple(sums)

        sums = lax.fori_loop(0, 4, step, (jnp.zeros((16, 128), F32),) * 4)
        a, b = sums[0] + sums[1], sums[2] + sums[3]
        own = lane16 == sub16
        re = jnp.sum(
            jnp.where(own, jnp.sum(a, axis=1, keepdims=True), 0.0), axis=0, keepdims=True
        )
        im = jnp.sum(
            jnp.where(own, jnp.sum(b, axis=1, keepdims=True), 0.0), axis=0, keepdims=True
        )
        cown[j, 0] = re + pltpu.roll(jnp.broadcast_to(im, (8, 128)), 16, axis=1)[0:1]
        for k, (dx, dy) in enumerate(DIRS):
            send(cown.at[j], crecv.at[j, pl.ds(7 - k, 1)], CX + j, towards[dx, dy])
        return re, im

    def spread(table, here):
        which = idx[here, :]
        return (
            jnp.take_along_axis(table, which, axis=1, mode="promise_in_bounds"),
            jnp.take_along_axis(table, which + 16, axis=1, mode="promise_in_bounds"),
        )

    def place(table, base):
        here = pl.ds(base, 8)
        a, b = spread(table, here)
        p[0, here, :] = a
        p[1, here, :] = b

    def clear_halo():
        def clear_tile(base):
            here = pl.ds(base, 8)
            p[0, here, :] = zero
            p[1, here, :] = zero

        over_halo(3, clear_tile)

    def over_halo(width, body):
        low = HALO - width
        body(row_of(low - 1, 4))
        for e in [*range(low, HALO), *range(HALO + NXD, HALO + NXD + width)]:
            for t in range(5):
                body(row_of(e, t))

        def edge(e):
            body(pl.multiple_of(row_of(e, 4), 8))

        over_rows(HALO, HALO + NXD, 8, edge)

    def prolong_own(j):
        table = jnp.broadcast_to(cown[j, 0], (8, 128))
        over_own(functools.partial(place, table))

    def prolong_halo(j):
        take(crecv.at[j], sem_r.at[CX + j])

        def row(dx, dy):
            if (dx, dy) == (0, 0):
                return jnp.broadcast_to(cown[j, 0], (8, 128))
            return jnp.broadcast_to(crecv[j, DIRS.index((dx, dy))], (8, 128))

        def side(e):
            return -1 if e < HALO else (1 if e >= HALO + NXD else 0)

        def halo_table(e):
            return jnp.where(sub < 4, row(side(e), 1), row(side(e + 1), -1))

        place(halo_table(-1), row_of(-1, 4))
        for e in [0, 1, 2, 19, 20, 21]:
            table = row(side(e), 0)
            for t in range(4):
                place(table, row_of(e, t))
            place(halo_table(e), row_of(e, 4))
        place(halo_table(18), row_of(18, 4))
        edge = halo_table(HALO)

        def middle(e):
            place(edge, pl.multiple_of(row_of(e, 4), 8))

        over_rows(3, 18, 5, middle)

    def send_halo(j):
        fields = [(u.at[j, 0], 2), (u.at[j, 1], 2)]
        cells = [(u.at[j, 0], 0, 0), (u.at[j, 1], 0, 0)]
        pack_y(uy_s.at[j], fields)
        pack_corners(uc_s.at[j], cells)
        send_x(fields, UX + j)
        send_y(uy_s.at[j], uy_r.at[j], UY + j)
        send_corners(uc_s.at[j], uc_r.at[j], UC + j)

    def take_halo(j):
        fields = [(u.at[j, 0], 2), (u.at[j, 1], 2)]
        cells = [(u.at[j, 0], 0, 0), (u.at[j, 1], 0, 0)]
        take(z.at[4, 0, pl.ds(0, 8 * NYD)], sem_r.at[UX + j])
        take(uy_r.at[j], sem_r.at[UY + j])
        take(uc_r.at[j], sem_r.at[UC + j])
        unpack_y(uy_r.at[j], fields)
        unpack_corners(uc_r.at[j], cells)

    def over_own(body):
        def row(x):
            for t in range(4):
                body(pl.multiple_of(row_of(x + HALO, t), 8))

        over_rows(0, NXD, 4, row)

    columns = []
    lengths = []
    coarse = []

    def finish(j, dots):
        squared = dots[0]
        col = [(dots[1 + 2 * i], dots[2 + 2 * i]) for i in range(j)]
        for re, im in col:
            squared = squared - (re * re + im * im)
        if j > 0:
            squared = jnp.maximum(squared, 0.0)
            columns.append(col)
        lengths.append(jnp.sqrt(squared + epsilon))

    for j in range(ITERS):
        smooth_all(j)
        start_gather(j, restrict(), products(j))
        if j + 1 < ITERS:
            send_halo(j)
        middle_gather(j)
        clear_halo()
        if j + 1 < ITERS:
            take_halo(j)
        dots = end_gather(j)
        coarse.append(coarse_solve(j))
        finish(j, dots)
        inverse = 1.0 / lengths[j]
        col = columns[j - 1] if j else []

        def make_basis(base):
            here = pl.ds(base, 8)
            a, b = z[j, 0, here, :], z[j, 1, here, :]
            for i, (re, im) in enumerate(col):
                c, d = v[i, 0, here, :], v[i, 1, here, :]
                a = a - (re * c - im * d)
                b = b - (re * d + im * c)
            v[j, 0, here, :] = a * inverse
            v[j, 1, here, :] = b * inverse

        def make_start(base):
            here = pl.ds(base, 8)
            a, b = u[j, 0, here, :], u[j, 1, here, :]
            for i, (re, im) in enumerate(col):
                c, d = z[i + 1, 0, here, :], z[i + 1, 1, here, :]
                a = a - (re * c - im * d)
                b = b - (re * d + im * c)
            z[j + 1, 0, here, :] = a
            z[j + 1, 1, here, :] = b

        if j + 1 < ITERS:
            over_tiles(2, make_start, 4)
        else:
            over_own(make_start)
        zn = z.at[j + 1]
        last = j + 1 == ITERS

        def make_image(base):
            here = pl.ds(base, 8)
            _, _, w0, w1 = operate(p, base)
            a, b = (zn[0, here, :] + w0) * inverse, (zn[1, here, :] + w1) * inverse
            zn[0, here, :] = a
            zn[1, here, :] = b
            if not last:
                put_first(here, a, b)

        prolong_own(j)
        over_own(make_image)
        over_own(make_basis)
        prolong_halo(j)
        if not last:
            over_halo(2, make_image)

        def add_edges(e, t, shifts):
            base = row_of(e, t)
            if not isinstance(e, int):
                base = pl.multiple_of(base, 8)
            here = pl.ds(base, 8)
            parts = [zn[0, here, :], zn[1, here, :]]
            for c in range(2):
                for shift in shifts:
                    beyond = p[c, pl.ds(base + shift, 8), :]
                    if shift == 1:
                        beyond = jnp.where(sub == 7, beyond, 0.0)
                    if shift == -1:
                        beyond = jnp.where(sub == 0, beyond, 0.0)
                    parts[c] = parts[c] - beyond * inverse
                zn[c, here, :] = parts[c]
            if not last:
                put_first(here, parts[0], parts[1])

        for e, shift in ((HALO, -PITCH), (HALO + NXD - 1, PITCH)):
            add_edges(e, 0, (shift, -1))
            add_edges(e, 1, (shift,))
            add_edges(e, 2, (shift,))
            add_edges(e, 3, (shift, 1))

        def y_edges(e):
            add_edges(e, 0, (-1,))
            add_edges(e, 3, (1,))

        over_rows(HALO + 1, HALO + NXD - 1, 7, y_edges)

    start_gather(ITERS, None, products(ITERS))
    middle_gather(ITERS)
    finish(ITERS, end_gather(ITERS))

    def times(a, b):
        return (a[0] * b[0] - a[1] * b[1], a[0] * b[1] + a[1] * b[0])

    def conj_times(a, b):
        return (a[0] * b[0] + a[1] * b[1], a[0] * b[1] - a[1] * b[0])

    rotations, upper, diagonal = [], [], []
    target = [(lengths[0], zero)]
    for j in range(ITERS):
        col = list(columns[j])
        for k, (c, s) in enumerate(rotations):
            head, tail = col[k], col[k + 1]
            turned = conj_times(c, head)
            other = times(c, tail)
            col[k] = (turned[0] + s * tail[0], turned[1] + s * tail[1])
            col[k + 1] = (other[0] - s * head[0], other[1] - s * head[1])
        below = lengths[j + 1]
        a = col[j]
        size = jnp.sqrt(a[0] * a[0] + a[1] * a[1] + below * below)
        c, s = (a[0] / size, a[1] / size), below / size
        rotations.append((c, s))
        upper.append(col)
        diagonal.append(size)
        last = target[j]
        target[j] = conj_times(c, last)
        target.append((-s * last[0], -s * last[1]))
    solved = [None] * ITERS
    for j in reversed(range(ITERS)):
        re, im = target[j]
        for k in range(j + 1, ITERS):
            part = times(upper[k][j], solved[k])
            re, im = re - part[0], im - part[1]
        solved[j] = (re / diagonal[j], im / diagonal[j])

    weights = [None] * ITERS
    for j in reversed(range(ITERS)):
        inverse = 1.0 / lengths[j]
        weights[j] = (solved[j][0] * inverse, solved[j][1] * inverse)
        if j:
            for i, h in enumerate(columns[j - 1]):
                part = times(h, weights[j])
                solved[i] = (solved[i][0] - part[0], solved[i][1] - part[1])

    c_re, c_im = zero, zero
    for j in range(ITERS):
        wr, wi = weights[j]
        c_re = c_re + (wr * coarse[j][0] - wi * coarse[j][1])
        c_im = c_im + (wr * coarse[j][1] + wi * coarse[j][0])
    table = c_re + pltpu.roll(c_im, 16, axis=1)

    def write(x):
        for t in range(4):
            here = pl.ds(pl.multiple_of(row_of(x + HALO, t), 8), 8)
            a, b = spread(table, here)
            for j in range(ITERS):
                wr, wi = weights[j]
                c, d = m[j, 0, here, :], m[j, 1, here, :]
                a = a + (wr * c - wi * d)
                b = b + (wr * d + wi * c)
            sol[0, x, pl.ds(8 * t, 8), :] = a
            sol[1, x, pl.ds(8 * t, 8), :] = b

    over_rows(0, NXD, 4, write)

    h_re, h_im = zero, zero
    for j in range(ITERS):
        for i, (re, im) in enumerate(columns[j]):
            spot = (sub == j) & (lane == i)
            h_re = jnp.where(spot, re, h_re)
            h_im = jnp.where(spot, im, h_im)
        h_re = jnp.where((sub == j) & (lane == j + 1), lengths[j + 1], h_re)
    hess[0] = h_re[:ITERS, : ITERS + 1]
    hess[1] = h_im[:ITERS, : ITERS + 1]

    take(u.at[0, 0, pl.ds(0, 22 * NYD)], sem_s.at[0])
    take(iy_s, sem_s.at[1])
    take(ic_s, sem_s.at[2])
    for j in range(ITERS + 1):
        take(g1.at[j, pl.ds(0, 30)], sem_s.at[S1 + j])
        take(g2.at[j, pl.ds(0, 75)], sem_s.at[S2 + j])
    for j in range(ITERS):
        take(crecv.at[j], sem_s.at[CX + j])
        if j + 1 < ITERS:
            take(z.at[4, 0, pl.ds(0, 8 * NYD)], sem_s.at[UX + j])
            take(uy_s.at[j], sem_s.at[UY + j])
            take(uc_s.at[j], sem_s.at[UC + j])


def body(*args):
    field = pltpu.VMEM((2, ROWS, 128), F32)
    plane = pltpu.VMEM((ROWS, 128), F32)

    def fields(n):
        return pltpu.VMEM((n, 2, ROWS, 128), F32)

    vmem = pl.BlockSpec(memory_space=pltpu.VMEM)
    solution, hessenberg = pl.pallas_call(
        kernel,
        out_shape=(
            jax.ShapeDtypeStruct(args[0].shape, F32),
            jax.ShapeDtypeStruct((2, ITERS, ITERS + 1), F32),
        ),
        in_specs=[pl.BlockSpec(memory_space=pl.ANY)] * 5,
        out_specs=(vmem, vmem),
        scratch_shapes=[
            *[pltpu.VMEM(a.shape, a.dtype) for a in args],
            *[plane] * 7,
            pltpu.VMEM((ROWS, 128), jnp.int32),
            fields(5), fields(4), fields(4), fields(4),
            field, field,
            pltpu.VMEM((2, NXD, NYD, 128), F32),
            pltpu.VMEM((64, 16, 128), F32),
            pltpu.VMEM((64, 16, 128), F32),
            pltpu.VMEM((5, 32, 1, 128), F32),
            pltpu.VMEM((5, 80, 1, 128), F32),
            pltpu.VMEM((4, 1, 1, 128), F32),
            pltpu.VMEM((4, 8, 1, 128), F32),
            pltpu.VMEM((2, 11, 16, 128), F32),
            pltpu.VMEM((2, 11, 16, 128), F32),
            pltpu.VMEM((4, 8, 128), F32),
            pltpu.VMEM((4, 8, 128), F32),
            pltpu.VMEM((3, 2, 4, 16, 128), F32),
            pltpu.VMEM((3, 2, 4, 16, 128), F32),
            pltpu.VMEM((3, 4, 8, 128), F32),
            pltpu.VMEM((3, 4, 8, 128), F32),
            pltpu.SemaphoreType.DMA((28,)),
            pltpu.SemaphoreType.DMA((28,)),
            pltpu.SemaphoreType.DMA((5,)),
        ],
        compiler_params=pltpu.CompilerParams(
            collective_id=0, has_side_effects=True, vmem_limit_bytes=60 * 1024 * 1024
        ),
    )(*args)
    return solution, hessenberg.transpose(0, 2, 1)


def solution(mesh):
    finer = Mesh(mesh.devices.reshape(2, 4, 2, 4, 4), AXES)
    in_specs = (
        P(None, GX, GY, None),
        P(GX, GY, None),
        P(GX, GY, None),
        P(GX, GY, None),
        P(None, GX + GY, None),
    )
    out_specs = (P(None, GX, GY, None), P())
    return jax.shard_map(body, mesh=finer, in_specs=in_specs, out_specs=out_specs, check_vma=False)
```

```python
import functools

import jax
import jax.numpy as jnp
from jax import lax
from jax.experimental import pallas as pl
from jax.experimental.pallas import tpu as pltpu
from jax.sharding import Mesh
from jax.sharding import PartitionSpec as P

ITERS = 4
AXES = ("zh", "px", "co", "py", "zl")
GX = ("zh", "px", "co")
GY = ("py", "zl")
damping = 0.8
pml_strength = 3.0
epsilon = 1e-06

FRONT = 8
PITCH = 40
HALO = 3
NXD = 16
NYD = 32
ROWS = FRONT + (NXD + 2 * HALO) * PITCH
MESH = pl.DeviceIdType.MESH
DIRS = [(-1, -1), (-1, 0), (-1, 1), (0, -1), (0, 1), (1, -1), (1, 0), (1, 1)]
CORNERS = [(-1, -1), (-1, 1), (1, -1), (1, 1)]
F32 = jnp.float32


def over_rows(low, high, group, body):
    def trip(k, carry):
        for q in range(group):
            body(low + k * group + q)
        return carry

    lax.fori_loop(0, (high - low) // group, trip, 0)


def row_of(e, t=0):
    return FRONT + e * PITCH + t * 8


def kernel(
    rhs_in, wave_in, layer_in, agg_in, cinv_in,
    sol, hess,
    rhs, wave, layer, agg, cinv,
    wv, lf, ag, dg, ab, sr, si, idx,
    z, u, m, v, f, p, rem, parts,
    dre, dim, g1, g2, cown, crecv,
    iy_s, iy_r, ic_s, ic_r, ly_s, ly_r, lc_s, lc_r, uy_s, uy_r, uc_s, uc_r,
    sem_s, sem_r, sem_in,
):
    zh, px, co = lax.axis_index("zh"), lax.axis_index("px"), lax.axis_index("co")
    py, zl = lax.axis_index("py"), lax.axis_index("zl")
    gx = zh * 8 + px * 2 + co
    gy = py * 4 + zl
    s1 = (zh * 2 + co) * 4 + zl
    s2 = px * 4 + py

    def device(a, b):
        return (
            lax.div(a, 8), lax.rem(lax.div(a, 2), 4), lax.rem(a, 2), lax.div(b, 4), lax.rem(b, 4)
        )

    def beside_device(dx, dy):
        return device(lax.rem(gx + 16 + dx, 16), lax.rem(gy + 16 + dy, 16))

    far = (2, 3, 1, 0)
    zhs = [zh, 1 - zh]
    cos = [co, 1 - co]
    zls = [zl] + [lax.rem(zl + k, 4) for k in range(1, 4)]
    pxs = [px] + [lax.rem(px + k, 4) for k in range(1, 4)]
    pys = [py] + [lax.rem(py + k, 4) for k in range(1, 4)]
    group1 = [
        (zhs[a], px, cos[b], py, zls[c])
        for a in (1, 0) for c in far for b in (1, 0) if (a, b, c) != (0, 0, 0)
    ]
    group2 = [
        (zh, pxs[a], co, pys[b], zl) for a in far for b in far if (a, b) != (0, 0)
    ]
    towards = {d: beside_device(*d) for d in DIRS}

    lane = lax.broadcasted_iota(jnp.int32, (8, 128), 1)
    sub = lax.broadcasted_iota(jnp.int32, (8, 128), 0)
    lane1 = lax.broadcasted_iota(jnp.int32, (1, 128), 1)
    zero = jnp.zeros((8, 128), F32)

    barrier = pltpu.get_barrier_semaphore()
    partners = group1 + group2 + list(towards.values())
    for target in partners:
        pl.semaphore_signal(barrier, inc=1, device_id=target, device_id_type=MESH)

    loads = [
        pltpu.make_async_copy(src, dst, sem_in.at[k])
        for k, (src, dst) in enumerate(
            [(wave_in, wave), (layer_in, layer), (agg_in, agg), (rhs_in, rhs), (cinv_in, cinv)]
        )
    ]
    for load in loads:
        load.start()

    def send(src, dst, kind, target):
        pltpu.make_async_remote_copy(
            src_ref=src,
            dst_ref=dst,
            send_sem=sem_s.at[kind],
            recv_sem=sem_r.at[kind],
            device_id=target,
            device_id_type=MESH,
        ).start()

    def take(like, sem):
        pltpu.make_async_copy(like, like, sem).wait()

    def coefficients(w, lay):
        wave_sq = w * w
        depth = lay / 3.0
        absorb = wave_sq * (pml_strength * depth * depth)
        diag = 6.0 - wave_sq
        magnitude = diag * diag + absorb * absorb
        return diag, absorb, damping * diag / magnitude, damping * absorb / magnitude

    for load in loads[:4]:
        load.wait()

    def own_rows(x):
        for t in range(4):
            here = pl.ds(pl.multiple_of(row_of(x + HALO, t), 8), 8)
            there = pl.ds(8 * t, 8)
            w = wave[x, there, :]
            lay = layer[x, there, :].astype(F32)
            which = agg[x, there, :]
            wv[here, :] = w
            lf[here, :] = lay
            ag[here, :] = which.astype(F32)
            idx[here, :] = which
            d, a, r, i = coefficients(w, lay)
            dg[here, :] = d
            ab[here, :] = a
            sr[here, :] = r
            si[here, :] = i
            z0, z1 = rhs[0, x, there, :], rhs[1, x, there, :]
            z[0, 0, here, :] = z0
            z[0, 1, here, :] = z1
            f[0, here, :] = r * z0 - i * z1
            f[1, here, :] = r * z1 + i * z0

    over_rows(0, NXD, 2, own_rows)

    def clear(k, carry):
        ag[pl.ds(pl.multiple_of(k * PITCH, 8), 8), :] = zero
        return carry

    lax.fori_loop(0, NXD + 2 * HALO + 1, clear, 0)

    def no_rows(first):
        for ref in (wv, lf, ag, *[r.at[c] for r in (f, z.at[0], u.at[0], u.at[1], u.at[2]) for c in (0, 1)]):
            for e in range(first, first + HALO):
                for t in range(4):
                    ref[pl.ds(row_of(e, t), 8), :] = zero

    pl.when(gx == 0)(lambda: no_rows(0))
    pl.when(gx == 15)(lambda: no_rows(HALO + NXD))

    def y_columns(ref, y):
        return ref[pl.ds(row_of(HALO) + y, NXD, stride=PITCH), :]

    def pack_y(buf, fields):
        for at, (ref, d) in enumerate(fields):
            buf[0, at] = y_columns(ref, d)
            buf[1, at] = y_columns(ref, NYD - 1 - d)

    def unpack_y(buf, fields, which):
        for at, (ref, d) in enumerate(fields):
            if which(at):
                ref[pl.ds(row_of(HALO) + NYD + d, NXD, stride=PITCH), :] = buf[0, at]
                ref[pl.ds(row_of(HALO) - 1 - d, NXD, stride=PITCH), :] = buf[1, at]

    def send_x(fields, kind):
        def rows(e):
            return pl.ds(row_of(e), NYD)

        @pl.when(gx > 0)
        def _():
            for ref, d in fields:
                send(
                    ref.at[rows(HALO + d)], ref.at[rows(HALO + NXD + d)], kind + 1, towards[-1, 0]
                )

        @pl.when(gx < 15)
        def _():
            for ref, d in fields:
                send(
                    ref.at[rows(HALO + NXD - 1 - d)], ref.at[rows(HALO - 1 - d)], kind,
                    towards[1, 0],
                )

    def take_x(fields, kind):
        like = u.at[0, 0, pl.ds(0, len(fields) * NYD)]
        pl.when(gx > 0)(lambda: take(like, sem_r.at[kind]))
        pl.when(gx < 15)(lambda: take(like, sem_r.at[kind + 1]))

    def take_sent_x(fields, kind):
        like = u.at[0, 0, pl.ds(0, len(fields) * NYD)]
        pl.when(gx > 0)(lambda: take(like, sem_s.at[kind + 1]))
        pl.when(gx < 15)(lambda: take(like, sem_s.at[kind]))

    def send_y(out, into, kind):
        send(out.at[0], into.at[0], kind, towards[0, -1])
        send(out.at[1], into.at[1], kind, towards[0, 1])

    def edge_row(dx, dy, ox, oy):
        x = ox if dx < 0 else NXD - 1 - ox
        y = oy if dy < 0 else NYD - 1 - oy
        return row_of(HALO + x) + y

    def past_row(dx, dy, ox, oy):
        x = -1 - ox if dx < 0 else NXD + ox
        y = -1 - oy if dy < 0 else NYD + oy
        return row_of(HALO + x) + y

    def pack_corners(buf, cells):
        for k, (dx, dy) in enumerate(CORNERS):
            for at, (ref, ox, oy) in enumerate(cells):
                buf[k, pl.ds(at, 1), :] = ref[pl.ds(edge_row(dx, dy, ox, oy), 1), :]

    def send_corners(out, into, kind):
        for k, (dx, dy) in enumerate(CORNERS):
            send(out.at[k], into.at[3 - k], kind, towards[dx, dy])

    def unpack_corners(buf, cells):
        for k, (dx, dy) in enumerate(CORNERS):
            for at, (ref, ox, oy) in enumerate(cells):
                ref[pl.ds(past_row(dx, dy, ox, oy), 1), :] = buf[k, pl.ds(at, 1), :]

    E0, E1, EU = 14, 18, 22
    soon = [(z.at[0, 0], 0), (z.at[0, 1], 0), (wv, 0), (lf, 0), (f.at[0], 1), (f.at[1], 1)]
    soon_cells = [(f.at[0], 0, 0), (f.at[1], 0, 0)]
    late = [(wv, 1), (lf, 1), (ag, 0), (ag, 1), (ag, 2)]
    late_cells = [(wv, 0, 0), (lf, 0, 0), (ag, 0, 0), (ag, 1, 0), (ag, 0, 1)]
    pack_y(iy_s, soon)
    pack_corners(ic_s, soon_cells)
    pack_y(ly_s, late)
    pack_corners(lc_s, late_cells)

    pl.semaphore_wait(barrier, len(partners))

    send_x(soon, E0)
    send_y(iy_s, iy_r, E0 + 2)
    send_corners(ic_s, ic_r, E0 + 3)
    send_x(late, E1)
    send_y(ly_s, ly_r, E1 + 2)
    send_corners(lc_s, lc_r, E1 + 3)

    lane16 = lax.broadcasted_iota(jnp.int32, (16, 128), 1)
    low16 = lane16 < 64

    def arrange(a, carry):
        at_a = lax.rem(lax.div(a, 2), 4) * 16 + lax.div(a, 8) * 2 + lax.rem(a, 2)
        for half in range(2):
            cols = pl.ds(pl.multiple_of(a * 256 + half * 128, 128), 128)
            c_re, c_im = cinv[0, :, cols], cinv[1, :, cols]
            r_re, r_im = pltpu.roll(c_re, 64, axis=1), pltpu.roll(c_im, 64, axis=1)
            at = at_a + (2 * half) * 4
            dre[at] = jnp.where(low16, c_re, -r_im)
            dim[at] = jnp.where(low16, c_im, r_re)
            dre[at + 4] = jnp.where(low16, r_re, -c_im)
            dim[at + 4] = jnp.where(low16, r_im, c_re)
        return carry

    loads[4].wait()
    lax.fori_loop(0, 16, arrange, 0)

    def x_inside(e):
        below = jnp.where(gx > 0, 1, 0)
        above = jnp.where(gx < 15, 1, 0)
        return jnp.where(e < HALO, below, jnp.where(e >= HALO + NXD, above, 1))

    y_up = jnp.where(gy < 15, 1, 0)
    y_down = jnp.where(gy > 0, 1, 0)

    def halo_tile(e, t, with_index, with_coefficients):
        base = row_of(e, t)
        here = pl.ds(base if isinstance(e, int) else pl.multiple_of(base, 8), 8)
        if t < 4:
            inside = jnp.full((8, 128), x_inside(e), jnp.int32) > 0
        else:
            inside = jnp.where(sub < 4, x_inside(e) * y_up, x_inside(e + 1) * y_down) > 0
        if with_index:
            idx[here, :] = jnp.where(inside, ag[here, :].astype(jnp.int32), 32)
        if with_coefficients:
            d, a, r, i = coefficients(wv[here, :], lf[here, :])
            dg[here, :] = d
            ab[here, :] = a
            sr[here, :] = jnp.where(inside, r, 0.0)
            si[here, :] = jnp.where(inside, i, 0.0)

    def each_halo(width, body):
        low = HALO - width
        body(low - 1, 4)
        for e in [*range(low, HALO), *range(HALO + NXD, HALO + NXD + width)]:
            for t in range(5):
                body(e, t)

        def edge(e):
            body(e, 4)

        over_rows(HALO, HALO + NXD, 8, edge)

    def over_halo(width, body):
        def tile(e, t):
            base = row_of(e, t)
            body(base if isinstance(e, int) else pl.multiple_of(base, 8))

        each_halo(width, tile)

    def put_first(here, a, b):
        r, i = sr[here, :], si[here, :]
        f[0, here, :] = r * a - i * b
        f[1, here, :] = r * b + i * a

    take_x(soon, E0)
    take(iy_r, sem_r.at[E0 + 2])
    take(ic_r, sem_r.at[E0 + 3])
    unpack_y(iy_r, soon, lambda at: at < 4)
    each_halo(1, lambda e, t: halo_tile(e, t, False, True))

    def halo_first(base):
        here = pl.ds(base, 8)
        put_first(here, z[0, 0, here, :], z[0, 1, here, :])

    over_halo(1, halo_first)
    unpack_y(iy_r, soon, lambda at: at >= 4)
    for k, (dx, dy) in enumerate(CORNERS):
        there = x_inside(-1 if dx < 0 else HALO + NXD) * (y_down if dy < 0 else y_up)
        there = jnp.full((8, 128), there, jnp.int32) > 0
        ic_r[k] = jnp.where(there, ic_r[k], 0.0)
    unpack_corners(ic_r, soon_cells)

    def take_late():
        take_sent_x(soon, E0)
        take_x(late, E1)
        take(ly_r, sem_r.at[E1 + 2])
        take(lc_r, sem_r.at[E1 + 3])
        unpack_y(ly_r, late, lambda at: True)
        unpack_corners(lc_r, late_cells)
        each_halo(2, lambda e, t: halo_tile(e, t, False, True))
        each_halo(3, lambda e, t: halo_tile(e, t, True, False))

    def neighbours(ref, c, base):
        centre = ref[c, pl.ds(base, 8), :]
        total = (
            ref[c, pl.ds(base + 1, 8), :]
            + ref[c, pl.ds(base - 1, 8), :]
            + ref[c, pl.ds(base + PITCH, 8), :]
            + ref[c, pl.ds(base - PITCH, 8), :]
        )
        up = jnp.where(lane == 127, 0.0, pltpu.roll(centre, 127, axis=1))
        down = jnp.where(lane == 0, 0.0, pltpu.roll(centre, 1, axis=1))
        return centre, total + up + down

    def operate(ref, base):
        c0, b0 = neighbours(ref, 0, base)
        c1, b1 = neighbours(ref, 1, base)
        here = pl.ds(base, 8)
        d, a = dg[here, :], ab[here, :]
        return c0, c1, d * c0 - b0 + a * c1, d * c1 - b1 - a * c0

    def over_tiles(width, body, group):
        low = HALO - width
        body(row_of(low - 1, 4))

        def row(e):
            for t in range(5):
                body(pl.multiple_of(row_of(e, t), 8))

        over_rows(low, HALO + NXD + width, group, row)

    four, five = (0, 1, 2, 3), (0, 1, 2, 3, 4)
    ALL = [(3, 19, 4, four)]
    INNER_SECOND = [(5, 17, 4, four)]
    OUTER_SECOND = [(2, 5, 3, five), (17, 20, 3, five), (5, 17, 4, (0, 3, 4))]
    INNER_REST = [(6, 16, 5, (1, 2))]
    OUTER_REST = [(3, 6, 3, four), (16, 19, 3, four), (6, 16, 5, (0, 3))]
    INNER_DOTS = [(4, 18, 7, (1, 2))]
    OUTER_DOTS = [(3, 4, 1, four), (18, 19, 1, four), (4, 18, 7, (0, 3))]

    def sweep(tiles, body):
        for low, high, group, ts in tiles:

            def row(e, ts=ts):
                for t in ts:
                    body(pl.multiple_of(row_of(e, t), 8), e, t)

            over_rows(low, high, group, row)

    def sweep_sums(tiles, sums, add):
        for low, high, group, ts in tiles:

            def trip(k, carry, low=low, group=group, ts=ts):
                carry = list(carry)
                for q in range(group):
                    for t in ts:
                        e = low + k * group + q
                        add(carry, pl.multiple_of(row_of(e, t), 8), e, t)
                return tuple(carry)

            sums = lax.fori_loop(0, (high - low) // group, trip, tuple(sums))
        return sums

    def there(e, t):
        return pl.ds(pl.multiple_of((e - HALO) * NYD + 8 * t, 8), 8)

    def make_second(j):
        def body(base, e=None, t=None):
            here = pl.ds(base, 8)
            f0, b0 = neighbours(f, 0, base)
            f1, b1 = neighbours(f, 1, base)
            r, i = sr[here, :], si[here, :]
            m[j, 0, here, :] = (2.0 - damping) * f0 + (r * b0 - i * b1)
            m[j, 1, here, :] = (2.0 - damping) * f1 + (r * b1 + i * b0)

        return body

    def make_rest(j):
        def body(base, e, t):
            here = pl.ds(base, 8)
            _, _, w0, w1 = operate(m.at[j], base)
            u[j, 0, here, :] = w0
            u[j, 1, here, :] = w1
            rem[0, there(e, t), :] = z[j, 0, here, :] - w0
            rem[1, there(e, t), :] = z[j, 1, here, :] - w1

        return body

    def add_restricted(sums, base, e, t):
        which = idx[pl.ds(base, 8), :]
        a, b = rem[0, there(e, t), :], rem[1, there(e, t), :]
        for g in range(16):
            mask = which == g
            sums[g] = sums[g] + jnp.where(mask, a, 0.0)
            sums[16 + g] = sums[16 + g] + jnp.where(mask, b, 0.0)

    def add_products(j):
        def add(sums, base, e, t):
            here = pl.ds(base, 8)
            a, b = z[j, 0, here, :], z[j, 1, here, :]
            sums[0] = sums[0] + (a * a + b * b)
            for i in range(j):
                c, d = v[i, 0, here, :], v[i, 1, here, :]
                sums[1 + 2 * i] = sums[1 + 2 * i] + (c * a + d * b)
                sums[2 + 2 * i] = sums[2 + 2 * i] + (c * b - d * a)

        return add

    def in_lanes(sums, lane_of):
        out = zero
        for k, total in enumerate(sums):
            out = out + jnp.where(
                lane == lane_of(k), jnp.sum(total, axis=1, keepdims=True), 0.0
            )
        return jnp.sum(out, axis=0, keepdims=True)

    def keep(sums, at):
        for k, total in enumerate(sums):
            parts[at + k] = total

    def kept(count, at):
        return [parts[at + k] for k in range(count)]

    def inner(j):
        if j < ITERS:
            sweep(INNER_SECOND, make_second(j))
            sweep(INNER_REST, make_rest(j))
            keep(sweep_sums(INNER_REST, [zero] * 32, add_restricted), 0)
        keep(sweep_sums(INNER_DOTS, [zero] * (1 + 2 * j), add_products(j)), 32)

    def outer(j):
        restricted = None
        if j == 0:
            over_tiles(1, make_second(0), 3)
            sweep(ALL, make_rest(0))
            restricted = sweep_sums(ALL, [zero] * 32, add_restricted)
            dots = sweep_sums(ALL, [zero], add_products(0))
        else:
            if j < ITERS:
                make_second(j)(row_of(1, 4))
                sweep(OUTER_SECOND, make_second(j))
                sweep(OUTER_REST, make_rest(j))
                restricted = sweep_sums(OUTER_REST, kept(32, 0), add_restricted)
            dots = sweep_sums(OUTER_DOTS, kept(1 + 2 * j, 32), add_products(j))
        if restricted is not None:
            restricted = in_lanes(restricted, lambda k: zl * 16 + (k // 16) * 64 + k % 16)
        start_gather(j, restricted, in_lanes(dots, lambda k: k))

    S1, S2, CX = 0, 5, 10

    def start_gather(j, coarse, dots):
        mine = g1.at[j, pl.ds(2 * s1, 2)]
        g1[j, 2 * s1] = coarse if coarse is not None else jnp.zeros((1, 128), F32)
        g1[j, 2 * s1 + 1] = dots

        for target in group1:
            send(mine, mine, S1 + j, target)

    def middle_gather(j):
        take(g1.at[j, pl.ds(0, 30)], sem_r.at[S1 + j])
        for q in range(4):
            g2[j, 5 * s2 + q] = (g1[j, 8 * q] + g1[j, 8 * q + 2]) + (
                g1[j, 8 * q + 4] + g1[j, 8 * q + 6]
            )
        total = g1[j, 1]
        for s in range(1, 16):
            total = total + g1[j, 2 * s + 1]
        g2[j, 5 * s2 + 4] = total
        mine = g2.at[j, pl.ds(5 * s2, 5)]

        for target in group2:
            send(mine, mine, S2 + j, target)

    def end_gather(j):
        take(g2.at[j, pl.ds(0, 75)], sem_r.at[S2 + j])

    def all_products(j):
        total = g2[j, 4]
        for s in range(1, 16):
            total = total + g2[j, 5 * s + 4]
        return [
            jnp.broadcast_to(
                jnp.sum(jnp.where(lane1 == k, total, 0.0), axis=1, keepdims=True), (8, 128)
            )
            for k in range(1 + 2 * j)
        ]

    sub16 = lax.broadcasted_iota(jnp.int32, (16, 128), 0)

    def coarse_solve(j):
        def step(k, sums):
            sums = list(sums)
            for o in range(4):
                for q in range(4):
                    row = g2[j, 20 * k + 5 * o + q]
                    at = 16 * k + 4 * o + q
                    sums[q % 2] = sums[q % 2] + dre[at] * row
                    sums[2 + q % 2] = sums[2 + q % 2] + dim[at] * row
            return tuple(sums)

        sums = lax.fori_loop(0, 4, step, (jnp.zeros((16, 128), F32),) * 4)
        a, b = sums[0] + sums[1], sums[2] + sums[3]
        a = jnp.sum(a, axis=1, keepdims=True)
        b = jnp.sum(b, axis=1, keepdims=True)
        both = jnp.where(lane16 == sub16, a, 0.0) + jnp.where(lane16 == sub16 + 16, b, 0.0)
        cown[j, 0] = jnp.sum(both, axis=0, keepdims=True)
        for k, (dx, dy) in enumerate(DIRS):
            send(cown.at[j], crecv.at[j, pl.ds(7 - k, 1)], CX + j, towards[dx, dy])

    def spread(table, here):
        which = idx[here, :]
        return (
            jnp.take_along_axis(table, which, axis=1, mode="promise_in_bounds"),
            jnp.take_along_axis(table, which + 16, axis=1, mode="promise_in_bounds"),
        )

    def place(table, base):
        here = pl.ds(base, 8)
        a, b = spread(table, here)
        p[0, here, :] = a
        p[1, here, :] = b

    def clear_halo():
        def clear_tile(base):
            here = pl.ds(base, 8)
            p[0, here, :] = zero
            p[1, here, :] = zero

        over_halo(3, clear_tile)

    def prolong_own(j):
        table = jnp.broadcast_to(cown[j, 0], (8, 128))
        over_own(functools.partial(place, table))

    def prolong_halo(j):
        take(crecv.at[j], sem_r.at[CX + j])

        def row(dx, dy):
            if (dx, dy) == (0, 0):
                return jnp.broadcast_to(cown[j, 0], (8, 128))
            return jnp.broadcast_to(crecv[j, DIRS.index((dx, dy))], (8, 128))

        def side(e):
            return -1 if e < HALO else (1 if e >= HALO + NXD else 0)

        def halo_table(e):
            return jnp.where(sub < 4, row(side(e), 1), row(side(e + 1), -1))

        place(halo_table(-1), row_of(-1, 4))
        for e in [0, 1, 2, 19, 20, 21]:
            table = row(side(e), 0)
            for t in range(4):
                place(table, row_of(e, t))
            place(halo_table(e), row_of(e, 4))
        place(halo_table(18), row_of(18, 4))
        edge = halo_table(HALO)

        def middle(e):
            place(edge, pl.multiple_of(row_of(e, 4), 8))

        over_rows(3, 18, 5, middle)

    def image_fields(j):
        return (
            [(u.at[j, c], d) for d in (0, 1) for c in (0, 1)],
            [(u.at[j, 0], 0, 0), (u.at[j, 1], 0, 0)],
        )

    def send_halo(j):
        fields, cells = image_fields(j)
        pack_y(uy_s.at[j], fields)
        pack_corners(uc_s.at[j], cells)
        send_x(fields, EU + 4 * j)
        send_y(uy_s.at[j], uy_r.at[j], EU + 4 * j + 2)
        send_corners(uc_s.at[j], uc_r.at[j], EU + 4 * j + 3)

    def take_halo(j):
        fields, cells = image_fields(j)
        take_x(fields, EU + 4 * j)
        take(uy_r.at[j], sem_r.at[EU + 4 * j + 2])
        take(uc_r.at[j], sem_r.at[EU + 4 * j + 3])
        unpack_y(uy_r.at[j], fields, lambda at: True)
        unpack_corners(uc_r.at[j], cells)

    def over_own(body):
        def row(x):
            for t in range(4):
                body(pl.multiple_of(row_of(x + HALO, t), 8))

        over_rows(0, NXD, 4, row)

    columns = []
    lengths = []

    def finish(j, dots):
        squared = dots[0]
        col = [(dots[1 + 2 * i], dots[2 + 2 * i]) for i in range(j)]
        for re, im in col:
            squared = squared - (re * re + im * im)
        if j > 0:
            squared = jnp.maximum(squared, 0.0)
            columns.append(col)
        lengths.append(jnp.sqrt(squared + epsilon))

    for j in range(ITERS):
        outer(j)
        if j + 1 < ITERS:
            send_halo(j)
        middle_gather(j)
        clear_halo()
        if j == 0:
            take_late()
        if j + 1 < ITERS:
            take_halo(j)
        end_gather(j)
        coarse_solve(j)
        finish(j, all_products(j))
        inverse = 1.0 / lengths[j]
        col = columns[j - 1] if j else []

        def make_basis(base):
            here = pl.ds(base, 8)
            a, b = z[j, 0, here, :], z[j, 1, here, :]
            for i, (re, im) in enumerate(col):
                c, d = v[i, 0, here, :], v[i, 1, here, :]
                a = a - (re * c - im * d)
                b = b - (re * d + im * c)
            v[j, 0, here, :] = a * inverse
            v[j, 1, here, :] = b * inverse

        def make_start(base):
            here = pl.ds(base, 8)
            a, b = u[j, 0, here, :], u[j, 1, here, :]
            for i, (re, im) in enumerate(col):
                c, d = z[i + 1, 0, here, :], z[i + 1, 1, here, :]
                a = a - (re * c - im * d)
                b = b - (re * d + im * c)
            z[j + 1, 0, here, :] = a
            z[j + 1, 1, here, :] = b

        if j + 1 < ITERS:
            over_tiles(2, make_start, 4)
        else:
            over_own(make_start)
        zn = z.at[j + 1]
        last = j + 1 == ITERS

        def make_image(base):
            here = pl.ds(base, 8)
            _, _, w0, w1 = operate(p, base)
            a, b = (zn[0, here, :] + w0) * inverse, (zn[1, here, :] + w1) * inverse
            zn[0, here, :] = a
            zn[1, here, :] = b
            if not last:
                put_first(here, a, b)

        prolong_own(j)
        over_own(make_image)
        over_own(make_basis)
        inner(j + 1)
        prolong_halo(j)
        if not last:
            over_halo(2, make_image)

        def add_edges(e, t, shifts):
            base = row_of(e, t)
            if not isinstance(e, int):
                base = pl.multiple_of(base, 8)
            here = pl.ds(base, 8)
            edge = [zn[0, here, :], zn[1, here, :]]
            for c in range(2):
                for shift in shifts:
                    beyond = p[c, pl.ds(base + shift, 8), :]
                    if shift == 1:
                        beyond = jnp.where(sub == 7, beyond, 0.0)
                    if shift == -1:
                        beyond = jnp.where(sub == 0, beyond, 0.0)
                    edge[c] = edge[c] - beyond * inverse
                zn[c, here, :] = edge[c]
            if not last:
                put_first(here, edge[0], edge[1])

        for e, shift in ((HALO, -PITCH), (HALO + NXD - 1, PITCH)):
            add_edges(e, 0, (shift, -1))
            add_edges(e, 1, (shift,))
            add_edges(e, 2, (shift,))
            add_edges(e, 3, (shift, 1))

        def y_edges(e):
            add_edges(e, 0, (-1,))
            add_edges(e, 3, (1,))

        over_rows(HALO + 1, HALO + NXD - 1, 7, y_edges)

    outer(ITERS)
    middle_gather(ITERS)

    def times(a, b):
        return (a[0] * b[0] - a[1] * b[1], a[0] * b[1] + a[1] * b[0])

    def conj_times(a, b):
        return (a[0] * b[0] + a[1] * b[1], a[0] * b[1] - a[1] * b[0])

    rotations, upper, diagonal = [], [], []
    target = [(lengths[0], zero)]

    def rotate(j):
        col = list(columns[j])
        for k, (c, s) in enumerate(rotations):
            head, tail = col[k], col[k + 1]
            turned = conj_times(c, head)
            other = times(c, tail)
            col[k] = (turned[0] + s * tail[0], turned[1] + s * tail[1])
            col[k + 1] = (other[0] - s * head[0], other[1] - s * head[1])
        below = lengths[j + 1]
        a = col[j]
        size = jnp.sqrt(a[0] * a[0] + a[1] * a[1] + below * below)
        c, s = (a[0] / size, a[1] / size), below / size
        rotations.append((c, s))
        upper.append(col)
        diagonal.append(size)
        last = target[j]
        target[j] = conj_times(c, last)
        target.append((-s * last[0], -s * last[1]))
    for j in range(ITERS - 1):
        rotate(j)
    end_gather(ITERS)
    finish(ITERS, all_products(ITERS))
    rotate(ITERS - 1)
    solved = [None] * ITERS
    for j in reversed(range(ITERS)):
        re, im = target[j]
        for k in range(j + 1, ITERS):
            part = times(upper[k][j], solved[k])
            re, im = re - part[0], im - part[1]
        solved[j] = (re / diagonal[j], im / diagonal[j])

    weights = [None] * ITERS
    for j in reversed(range(ITERS)):
        inverse = 1.0 / lengths[j]
        weights[j] = (solved[j][0] * inverse, solved[j][1] * inverse)
        if j:
            for i, h in enumerate(columns[j - 1]):
                part = times(h, weights[j])
                solved[i] = (solved[i][0] - part[0], solved[i][1] - part[1])

    c_re, c_im = zero, zero
    for j in range(ITERS):
        wr, wi = weights[j]
        row = jnp.broadcast_to(cown[j, 0], (8, 128))
        c_re = c_re + wr * row
        c_im = c_im + wi * row
    turned = jnp.where(lane < 16, -pltpu.roll(c_im, 112, axis=1), pltpu.roll(c_im, 16, axis=1))
    table = jnp.where(lane < 32, c_re + turned, 0.0)

    def write(x):
        for t in range(4):
            here = pl.ds(pl.multiple_of(row_of(x + HALO, t), 8), 8)
            a, b = spread(table, here)
            for j in range(ITERS):
                wr, wi = weights[j]
                c, d = m[j, 0, here, :], m[j, 1, here, :]
                a = a + (wr * c - wi * d)
                b = b + (wr * d + wi * c)
            sol[0, x, pl.ds(8 * t, 8), :] = a
            sol[1, x, pl.ds(8 * t, 8), :] = b

    over_rows(0, NXD, 4, write)

    h_re, h_im = zero, zero
    for j in range(ITERS):
        for i, (re, im) in enumerate(columns[j]):
            spot = (sub == j) & (lane == i)
            h_re = jnp.where(spot, re, h_re)
            h_im = jnp.where(spot, im, h_im)
        h_re = jnp.where((sub == j) & (lane == j + 1), lengths[j + 1], h_re)
    hess[0] = h_re[:ITERS, : ITERS + 1]
    hess[1] = h_im[:ITERS, : ITERS + 1]

    for fields, kind, y_out, c_out in ((soon, E0, iy_s, ic_s), (late, E1, ly_s, lc_s)):
        if kind != E0:
            take_sent_x(fields, kind)
        take(y_out, sem_s.at[kind + 2])
        take(c_out, sem_s.at[kind + 3])
    for j in range(ITERS + 1):
        take(g1.at[j, pl.ds(0, 30)], sem_s.at[S1 + j])
        take(g2.at[j, pl.ds(0, 75)], sem_s.at[S2 + j])
    for j in range(ITERS):
        take(crecv.at[j], sem_s.at[CX + j])
        if j + 1 < ITERS:
            take_sent_x(image_fields(j)[0], EU + 4 * j)
            take(uy_s.at[j], sem_s.at[EU + 4 * j + 2])
            take(uc_s.at[j], sem_s.at[EU + 4 * j + 3])


def body(*args):
    field = pltpu.VMEM((2, ROWS, 128), F32)
    plane = pltpu.VMEM((ROWS, 128), F32)

    def fields(n):
        return pltpu.VMEM((n, 2, ROWS, 128), F32)

    vmem = pl.BlockSpec(memory_space=pltpu.VMEM)
    solution, hessenberg = pl.pallas_call(
        kernel,
        out_shape=(
            pltpu.VMEM(args[0].shape, F32),
            pltpu.VMEM((2, ITERS, ITERS + 1), F32),
        ),
        in_specs=[pl.BlockSpec(memory_space=pl.ANY)] * 5,
        out_specs=(vmem, vmem),
        scratch_shapes=[
            *[pltpu.VMEM(a.shape, a.dtype) for a in args],
            *[plane] * 7,
            pltpu.VMEM((ROWS, 128), jnp.int32),
            fields(5), fields(4), fields(4), fields(4),
            field, field,
            pltpu.VMEM((2, NXD * NYD, 128), F32),
            pltpu.VMEM((48, 8, 128), F32),
            pltpu.VMEM((64, 16, 128), F32),
            pltpu.VMEM((64, 16, 128), F32),
            pltpu.VMEM((5, 32, 1, 128), F32),
            pltpu.VMEM((5, 80, 1, 128), F32),
            pltpu.VMEM((4, 1, 1, 128), F32),
            pltpu.VMEM((4, 8, 1, 128), F32),
            pltpu.VMEM((2, 6, 16, 128), F32),
            pltpu.VMEM((2, 6, 16, 128), F32),
            pltpu.VMEM((4, 8, 128), F32),
            pltpu.VMEM((4, 8, 128), F32),
            pltpu.VMEM((2, 5, 16, 128), F32),
            pltpu.VMEM((2, 5, 16, 128), F32),
            pltpu.VMEM((4, 8, 128), F32),
            pltpu.VMEM((4, 8, 128), F32),
            pltpu.VMEM((3, 2, 4, 16, 128), F32),
            pltpu.VMEM((3, 2, 4, 16, 128), F32),
            pltpu.VMEM((3, 4, 8, 128), F32),
            pltpu.VMEM((3, 4, 8, 128), F32),
            pltpu.SemaphoreType.DMA((34,)),
            pltpu.SemaphoreType.DMA((34,)),
            pltpu.SemaphoreType.DMA((5,)),
        ],
        compiler_params=pltpu.CompilerParams(
            collective_id=0, has_side_effects=True, vmem_limit_bytes=60 * 1024 * 1024
        ),
    )(*args)
    return solution, hessenberg.transpose(0, 2, 1)


def solution(mesh):
    finer = Mesh(mesh.devices.reshape(2, 4, 2, 4, 4), AXES)
    in_specs = (
        P(None, GX, GY, None),
        P(GX, GY, None),
        P(GX, GY, None),
        P(GX, GY, None),
        P(None, GX + GY, None),
    )
    out_specs = (P(None, GX, GY, None), P())
    return jax.shard_map(body, mesh=finer, in_specs=in_specs, out_specs=out_specs, check_vma=False)
```

```python
import functools

import jax
import jax.numpy as jnp
from jax import lax
from jax.experimental import pallas as pl
from jax.experimental.pallas import tpu as pltpu
from jax.sharding import Mesh
from jax.sharding import PartitionSpec as P

ITERS = 4
AXES = ("zh", "px", "co", "py", "zl")
GX = ("zh", "px", "co")
GY = ("py", "zl")
damping = 0.8
pml_strength = 3.0
epsilon = 1e-06

FRONT = 8
PITCH = 40
HALO = 3
NXD = 16
NYD = 32
ROWS = FRONT + (NXD + 2 * HALO) * PITCH
MESH = pl.DeviceIdType.MESH
DIRS = [(-1, -1), (-1, 0), (-1, 1), (0, -1), (0, 1), (1, -1), (1, 0), (1, 1)]
CORNERS = [(-1, -1), (-1, 1), (1, -1), (1, 1)]
F32 = jnp.float32


def over_rows(low, high, group, body):
    def trip(k, carry):
        for q in range(group):
            body(low + k * group + q)
        return carry

    lax.fori_loop(0, (high - low) // group, trip, 0)


def row_of(e, t=0):
    return FRONT + e * PITCH + t * 8


def kernel(
    rhs_in, wave_in, layer_in, agg_in, cinv_in,
    sol, hess,
    rhs, wave, layer, agg, cinv,
    wv, lf, ag, dg, ab, sr, si, idx,
    z, u, m, v, f, p, rem, parts,
    dre, dim, g1, g2, cown, crecv,
    iy_s, iy_r, ic_s, ic_r, ly_s, ly_r, lc_s, lc_r, uy_s, uy_r, uc_s, uc_r,
    sem_s, sem_r, sem_in,
):
    zh, px, co = lax.axis_index("zh"), lax.axis_index("px"), lax.axis_index("co")
    py, zl = lax.axis_index("py"), lax.axis_index("zl")
    gx = zh * 8 + px * 2 + co
    gy = py * 4 + zl
    s1 = (zh * 2 + co) * 4 + zl
    s2 = px * 4 + py

    def device(a, b):
        return (
            lax.div(a, 8), lax.rem(lax.div(a, 2), 4), lax.rem(a, 2), lax.div(b, 4), lax.rem(b, 4)
        )

    def beside_device(dx, dy):
        return device(lax.rem(gx + 16 + dx, 16), lax.rem(gy + 16 + dy, 16))

    far = (2, 3, 1, 0)
    zhs = [zh, 1 - zh]
    cos = [co, 1 - co]
    zls = [zl] + [lax.rem(zl + k, 4) for k in range(1, 4)]
    pxs = [px] + [lax.rem(px + k, 4) for k in range(1, 4)]
    pys = [py] + [lax.rem(py + k, 4) for k in range(1, 4)]
    group1 = [
        (zhs[a], px, cos[b], py, zls[c])
        for a in (1, 0) for c in far for b in (1, 0) if (a, b, c) != (0, 0, 0)
    ]
    group2 = [
        (zh, pxs[a], co, pys[b], zl) for a in far for b in far if (a, b) != (0, 0)
    ]
    towards = {d: beside_device(*d) for d in DIRS}

    lane = lax.broadcasted_iota(jnp.int32, (8, 128), 1)
    sub = lax.broadcasted_iota(jnp.int32, (8, 128), 0)
    lane1 = lax.broadcasted_iota(jnp.int32, (1, 128), 1)
    zero = jnp.zeros((8, 128), F32)

    barrier = pltpu.get_barrier_semaphore()
    partners = group1 + group2 + list(towards.values())
    for target in partners:
        pl.semaphore_signal(barrier, inc=1, device_id=target, device_id_type=MESH)

    loads = [
        pltpu.make_async_copy(src, dst, sem_in.at[k])
        for k, (src, dst) in enumerate(
            [(wave_in, wave), (layer_in, layer), (agg_in, agg), (rhs_in, rhs), (cinv_in, cinv)]
        )
    ]
    for load in loads:
        load.start()

    def send(src, dst, kind, target):
        pltpu.make_async_remote_copy(
            src_ref=src,
            dst_ref=dst,
            send_sem=sem_s.at[kind],
            recv_sem=sem_r.at[kind],
            device_id=target,
            device_id_type=MESH,
        ).start()

    def take(like, sem):
        pltpu.make_async_copy(like, like, sem).wait()

    def coefficients(w, lay):
        wave_sq = w * w
        depth = lay / 3.0
        absorb = wave_sq * (pml_strength * depth * depth)
        diag = 6.0 - wave_sq
        magnitude = diag * diag + absorb * absorb
        return diag, absorb, damping * diag / magnitude, damping * absorb / magnitude

    for load in loads[:4]:
        load.wait()

    def own_rows(x):
        for t in range(4):
            here = pl.ds(pl.multiple_of(row_of(x + HALO, t), 8), 8)
            there = pl.ds(8 * t, 8)
            w = wave[x, there, :]
            lay = layer[x, there, :].astype(F32)
            which = agg[x, there, :]
            wv[here, :] = w
            lf[here, :] = lay
            ag[here, :] = which.astype(F32)
            idx[here, :] = which
            d, a, r, i = coefficients(w, lay)
            dg[here, :] = d
            ab[here, :] = a
            sr[here, :] = r
            si[here, :] = i
            z0, z1 = rhs[0, x, there, :], rhs[1, x, there, :]
            z[0, 0, here, :] = z0
            z[0, 1, here, :] = z1
            f[0, here, :] = r * z0 - i * z1
            f[1, here, :] = r * z1 + i * z0

    over_rows(0, NXD, 2, own_rows)

    def clear(k, carry):
        ag[pl.ds(pl.multiple_of(k * PITCH, 8), 8), :] = zero
        return carry

    lax.fori_loop(0, NXD + 2 * HALO + 1, clear, 0)

    def no_rows(first):
        for ref in (wv, lf, ag, *[r.at[c] for r in (f, z.at[0], u.at[0], u.at[1], u.at[2]) for c in (0, 1)]):
            for e in range(first, first + HALO):
                for t in range(4):
                    ref[pl.ds(row_of(e, t), 8), :] = zero

    pl.when(gx == 0)(lambda: no_rows(0))
    pl.when(gx == 15)(lambda: no_rows(HALO + NXD))

    def y_columns(ref, y):
        return ref[pl.ds(row_of(HALO) + y, NXD, stride=PITCH), :]

    def pack_y(buf, fields):
        for at, (ref, d) in enumerate(fields):
            buf[0, at] = y_columns(ref, d)
            buf[1, at] = y_columns(ref, NYD - 1 - d)

    def unpack_y(buf, fields, which):
        for at, (ref, d) in enumerate(fields):
            if which(at):
                ref[pl.ds(row_of(HALO) + NYD + d, NXD, stride=PITCH), :] = buf[0, at]
                ref[pl.ds(row_of(HALO) - 1 - d, NXD, stride=PITCH), :] = buf[1, at]

    def send_x(fields, kind):
        def rows(e):
            return pl.ds(row_of(e), NYD)

        @pl.when(gx > 0)
        def _():
            for ref, d in fields:
                send(
                    ref.at[rows(HALO + d)], ref.at[rows(HALO + NXD + d)], kind + 1, towards[-1, 0]
                )

        @pl.when(gx < 15)
        def _():
            for ref, d in fields:
                send(
                    ref.at[rows(HALO + NXD - 1 - d)], ref.at[rows(HALO - 1 - d)], kind,
                    towards[1, 0],
                )

    def take_x(fields, kind):
        like = u.at[0, 0, pl.ds(0, len(fields) * NYD)]
        pl.when(gx > 0)(lambda: take(like, sem_r.at[kind]))
        pl.when(gx < 15)(lambda: take(like, sem_r.at[kind + 1]))

    def take_sent_x(fields, kind):
        like = u.at[0, 0, pl.ds(0, len(fields) * NYD)]
        pl.when(gx > 0)(lambda: take(like, sem_s.at[kind + 1]))
        pl.when(gx < 15)(lambda: take(like, sem_s.at[kind]))

    def send_y(out, into, kind):
        send(out.at[0], into.at[0], kind, towards[0, -1])
        send(out.at[1], into.at[1], kind, towards[0, 1])

    def edge_row(dx, dy, ox, oy):
        x = ox if dx < 0 else NXD - 1 - ox
        y = oy if dy < 0 else NYD - 1 - oy
        return row_of(HALO + x) + y

    def past_row(dx, dy, ox, oy):
        x = -1 - ox if dx < 0 else NXD + ox
        y = -1 - oy if dy < 0 else NYD + oy
        return row_of(HALO + x) + y

    def pack_corners(buf, cells):
        for k, (dx, dy) in enumerate(CORNERS):
            for at, (ref, ox, oy) in enumerate(cells):
                buf[k, pl.ds(at, 1), :] = ref[pl.ds(edge_row(dx, dy, ox, oy), 1), :]

    def send_corners(out, into, kind):
        for k, (dx, dy) in enumerate(CORNERS):
            send(out.at[k], into.at[3 - k], kind, towards[dx, dy])

    def unpack_corners(buf, cells):
        for k, (dx, dy) in enumerate(CORNERS):
            for at, (ref, ox, oy) in enumerate(cells):
                ref[pl.ds(past_row(dx, dy, ox, oy), 1), :] = buf[k, pl.ds(at, 1), :]

    E0, E1, EU = 14, 18, 22
    soon = [(z.at[0, 0], 0), (z.at[0, 1], 0), (wv, 0), (lf, 0), (f.at[0], 1), (f.at[1], 1)]
    soon_cells = [(f.at[0], 0, 0), (f.at[1], 0, 0)]
    late = [(wv, 1), (lf, 1), (ag, 0), (ag, 1), (ag, 2)]
    late_cells = [(wv, 0, 0), (lf, 0, 0), (ag, 0, 0), (ag, 1, 0), (ag, 0, 1)]
    pack_y(iy_s, soon)
    pack_corners(ic_s, soon_cells)
    pack_y(ly_s, late)
    pack_corners(lc_s, late_cells)

    pl.semaphore_wait(barrier, len(partners))

    send_x(soon, E0)
    send_y(iy_s, iy_r, E0 + 2)
    send_corners(ic_s, ic_r, E0 + 3)
    send_x(late, E1)
    send_y(ly_s, ly_r, E1 + 2)
    send_corners(lc_s, lc_r, E1 + 3)

    lane16 = lax.broadcasted_iota(jnp.int32, (16, 128), 1)
    low16 = lane16 < 64

    def arrange(a, carry):
        at_a = lax.rem(lax.div(a, 2), 4) * 16 + lax.div(a, 8) * 2 + lax.rem(a, 2)
        for half in range(2):
            cols = pl.ds(pl.multiple_of(a * 256 + half * 128, 128), 128)
            c_re, c_im = cinv[0, :, cols], cinv[1, :, cols]
            r_re, r_im = pltpu.roll(c_re, 64, axis=1), pltpu.roll(c_im, 64, axis=1)
            at = at_a + (2 * half) * 4
            dre[at] = jnp.where(low16, c_re, -r_im)
            dim[at] = jnp.where(low16, c_im, r_re)
            dre[at + 4] = jnp.where(low16, r_re, -c_im)
            dim[at + 4] = jnp.where(low16, r_im, c_re)
        return carry

    loads[4].wait()
    lax.fori_loop(0, 16, arrange, 0)

    def x_inside(e):
        below = jnp.where(gx > 0, 1, 0)
        above = jnp.where(gx < 15, 1, 0)
        return jnp.where(e < HALO, below, jnp.where(e >= HALO + NXD, above, 1))

    y_up = jnp.where(gy < 15, 1, 0)
    y_down = jnp.where(gy > 0, 1, 0)

    def halo_tile(e, t, with_index, with_coefficients):
        base = row_of(e, t)
        here = pl.ds(base if isinstance(e, int) else pl.multiple_of(base, 8), 8)
        if t < 4:
            inside = jnp.full((8, 128), x_inside(e), jnp.int32) > 0
        else:
            inside = jnp.where(sub < 4, x_inside(e) * y_up, x_inside(e + 1) * y_down) > 0
        if with_index:
            idx[here, :] = jnp.where(inside, ag[here, :].astype(jnp.int32), 32)
        if with_coefficients:
            d, a, r, i = coefficients(wv[here, :], lf[here, :])
            dg[here, :] = d
            ab[here, :] = a
            sr[here, :] = jnp.where(inside, r, 0.0)
            si[here, :] = jnp.where(inside, i, 0.0)

    def each_halo(width, body):
        low = HALO - width
        body(low - 1, 4)
        for e in [*range(low, HALO), *range(HALO + NXD, HALO + NXD + width)]:
            for t in range(5):
                body(e, t)

        def edge(e):
            body(e, 4)

        over_rows(HALO, HALO + NXD, 8, edge)

    def over_halo(width, body):
        def tile(e, t):
            base = row_of(e, t)
            body(base if isinstance(e, int) else pl.multiple_of(base, 8))

        each_halo(width, tile)

    def put_first(here, a, b):
        r, i = sr[here, :], si[here, :]
        f[0, here, :] = r * a - i * b
        f[1, here, :] = r * b + i * a

    def take_late():
        take_sent_x(soon, E0)
        take_x(late, E1)
        take(ly_r, sem_r.at[E1 + 2])
        take(lc_r, sem_r.at[E1 + 3])
        unpack_y(ly_r, late, lambda at: True)
        unpack_corners(lc_r, late_cells)
        each_halo(2, lambda e, t: halo_tile(e, t, False, True))
        each_halo(3, lambda e, t: halo_tile(e, t, True, False))

    def neighbours(ref, c, base):
        centre = ref[c, pl.ds(base, 8), :]
        total = (
            ref[c, pl.ds(base + 1, 8), :]
            + ref[c, pl.ds(base - 1, 8), :]
            + ref[c, pl.ds(base + PITCH, 8), :]
            + ref[c, pl.ds(base - PITCH, 8), :]
        )
        up = jnp.where(lane == 127, 0.0, pltpu.roll(centre, 127, axis=1))
        down = jnp.where(lane == 0, 0.0, pltpu.roll(centre, 1, axis=1))
        return centre, total + up + down

    def operate(ref, base):
        c0, b0 = neighbours(ref, 0, base)
        c1, b1 = neighbours(ref, 1, base)
        here = pl.ds(base, 8)
        d, a = dg[here, :], ab[here, :]
        return c0, c1, d * c0 - b0 + a * c1, d * c1 - b1 - a * c0

    def over_tiles(width, body, group):
        low = HALO - width
        body(row_of(low - 1, 4))

        def row(e):
            for t in range(5):
                body(pl.multiple_of(row_of(e, t), 8))

        over_rows(low, HALO + NXD + width, group, row)

    four, five = (0, 1, 2, 3), (0, 1, 2, 3, 4)
    INNER_SECOND = [(5, 17, 4, four)]
    OUTER_SECOND = [(2, 5, 3, five), (17, 20, 3, five), (5, 17, 4, (0, 3, 4))]
    INNER_REST = [(6, 16, 5, (1, 2))]
    OUTER_REST = [(3, 6, 3, four), (16, 19, 3, four), (6, 16, 5, (0, 3))]
    INNER_DOTS = [(4, 18, 7, (1, 2))]
    OUTER_DOTS = [(3, 4, 1, four), (18, 19, 1, four), (4, 18, 7, (0, 3))]

    def sweep(tiles, body):
        for low, high, group, ts in tiles:

            def row(e, ts=ts):
                for t in ts:
                    body(pl.multiple_of(row_of(e, t), 8), e, t)

            over_rows(low, high, group, row)

    def sweep_sums(tiles, sums, add):
        for low, high, group, ts in tiles:

            def trip(k, carry, low=low, group=group, ts=ts):
                carry = list(carry)
                for q in range(group):
                    for t in ts:
                        e = low + k * group + q
                        add(carry, pl.multiple_of(row_of(e, t), 8), e, t)
                return tuple(carry)

            sums = lax.fori_loop(0, (high - low) // group, trip, tuple(sums))
        return sums

    def there(e, t):
        return pl.ds(pl.multiple_of((e - HALO) * NYD + 8 * t, 8), 8)

    def make_second(j):
        def body(base, e=None, t=None):
            here = pl.ds(base, 8)
            f0, b0 = neighbours(f, 0, base)
            f1, b1 = neighbours(f, 1, base)
            r, i = sr[here, :], si[here, :]
            m[j, 0, here, :] = (2.0 - damping) * f0 + (r * b0 - i * b1)
            m[j, 1, here, :] = (2.0 - damping) * f1 + (r * b1 + i * b0)

        return body

    def make_rest(j):
        def body(base, e, t):
            here = pl.ds(base, 8)
            _, _, w0, w1 = operate(m.at[j], base)
            u[j, 0, here, :] = w0
            u[j, 1, here, :] = w1
            rem[0, there(e, t), :] = z[j, 0, here, :] - w0
            rem[1, there(e, t), :] = z[j, 1, here, :] - w1

        return body

    def add_restricted(sums, base, e, t):
        which = idx[pl.ds(base, 8), :]
        a, b = rem[0, there(e, t), :], rem[1, there(e, t), :]
        for g in range(16):
            mask = which == g
            sums[g] = sums[g] + jnp.where(mask, a, 0.0)
            sums[16 + g] = sums[16 + g] + jnp.where(mask, b, 0.0)

    def add_products(j):
        def add(sums, base, e, t):
            here = pl.ds(base, 8)
            a, b = z[j, 0, here, :], z[j, 1, here, :]
            sums[0] = sums[0] + (a * a + b * b)
            for i in range(j):
                c, d = v[i, 0, here, :], v[i, 1, here, :]
                sums[1 + 2 * i] = sums[1 + 2 * i] + (c * a + d * b)
                sums[2 + 2 * i] = sums[2 + 2 * i] + (c * b - d * a)

        return add

    def in_lanes(sums, lane_of):
        out = zero
        for k, total in enumerate(sums):
            out = out + jnp.where(
                lane == lane_of(k), jnp.sum(total, axis=1, keepdims=True), 0.0
            )
        return jnp.sum(out, axis=0, keepdims=True)

    def keep(sums, at):
        for k, total in enumerate(sums):
            parts[at + k] = total

    def kept(count, at):
        return [parts[at + k] for k in range(count)]

    def inner(j):
        if j < ITERS:
            sweep(INNER_SECOND, make_second(j))
            sweep(INNER_REST, make_rest(j))
            keep(sweep_sums(INNER_REST, [zero] * 32, add_restricted), 0)
        keep(sweep_sums(INNER_DOTS, [zero] * (1 + 2 * j), add_products(j)), 32)

    def outer(j):
        restricted = None
        if j < ITERS:
            make_second(j)(row_of(1, 4))
            sweep(OUTER_SECOND, make_second(j))
            sweep(OUTER_REST, make_rest(j))
            restricted = sweep_sums(OUTER_REST, kept(32, 0), add_restricted)
        dots = sweep_sums(OUTER_DOTS, kept(1 + 2 * j, 32), add_products(j))
        if restricted is not None:
            restricted = in_lanes(restricted, lambda k: zl * 16 + (k // 16) * 64 + k % 16)
        start_gather(j, restricted, in_lanes(dots, lambda k: k))

    S1, S2, CX = 0, 5, 10

    def start_gather(j, coarse, dots):
        mine = g1.at[j, pl.ds(2 * s1, 2)]
        g1[j, 2 * s1] = coarse if coarse is not None else jnp.zeros((1, 128), F32)
        g1[j, 2 * s1 + 1] = dots

        for target in group1:
            send(mine, mine, S1 + j, target)

    def middle_gather(j):
        take(g1.at[j, pl.ds(0, 30)], sem_r.at[S1 + j])
        for q in range(4):
            g2[j, 5 * s2 + q] = (g1[j, 8 * q] + g1[j, 8 * q + 2]) + (
                g1[j, 8 * q + 4] + g1[j, 8 * q + 6]
            )
        total = g1[j, 1]
        for s in range(1, 16):
            total = total + g1[j, 2 * s + 1]
        g2[j, 5 * s2 + 4] = total
        mine = g2.at[j, pl.ds(5 * s2, 5)]

        for target in group2:
            send(mine, mine, S2 + j, target)

    def end_gather(j):
        take(g2.at[j, pl.ds(0, 75)], sem_r.at[S2 + j])

    def all_products(j):
        total = g2[j, 4]
        for s in range(1, 16):
            total = total + g2[j, 5 * s + 4]
        return [
            jnp.broadcast_to(
                jnp.sum(jnp.where(lane1 == k, total, 0.0), axis=1, keepdims=True), (8, 128)
            )
            for k in range(1 + 2 * j)
        ]

    sub16 = lax.broadcasted_iota(jnp.int32, (16, 128), 0)

    def coarse_solve(j):
        def step(k, sums):
            sums = list(sums)
            for o in range(4):
                for q in range(4):
                    row = g2[j, 20 * k + 5 * o + q]
                    at = 16 * k + 4 * o + q
                    sums[q % 2] = sums[q % 2] + dre[at] * row
                    sums[2 + q % 2] = sums[2 + q % 2] + dim[at] * row
            return tuple(sums)

        sums = lax.fori_loop(0, 4, step, (jnp.zeros((16, 128), F32),) * 4)
        a, b = sums[0] + sums[1], sums[2] + sums[3]
        a = jnp.sum(a, axis=1, keepdims=True)
        b = jnp.sum(b, axis=1, keepdims=True)
        both = jnp.where(lane16 == sub16, a, 0.0) + jnp.where(lane16 == sub16 + 16, b, 0.0)
        cown[j, 0] = jnp.sum(both, axis=0, keepdims=True)
        for k, (dx, dy) in enumerate(DIRS):
            send(cown.at[j], crecv.at[j, pl.ds(7 - k, 1)], CX + j, towards[dx, dy])

    def spread(table, here):
        which = idx[here, :]
        return (
            jnp.take_along_axis(table, which, axis=1, mode="promise_in_bounds"),
            jnp.take_along_axis(table, which + 16, axis=1, mode="promise_in_bounds"),
        )

    def place(table, base):
        here = pl.ds(base, 8)
        a, b = spread(table, here)
        p[0, here, :] = a
        p[1, here, :] = b

    def clear_halo():
        def clear_tile(base):
            here = pl.ds(base, 8)
            p[0, here, :] = zero
            p[1, here, :] = zero

        over_halo(3, clear_tile)

    def prolong_own(j):
        table = jnp.broadcast_to(cown[j, 0], (8, 128))
        over_own(functools.partial(place, table))

    def prolong_halo(j):
        take(crecv.at[j], sem_r.at[CX + j])

        def row(dx, dy):
            if (dx, dy) == (0, 0):
                return jnp.broadcast_to(cown[j, 0], (8, 128))
            return jnp.broadcast_to(crecv[j, DIRS.index((dx, dy))], (8, 128))

        def side(e):
            return -1 if e < HALO else (1 if e >= HALO + NXD else 0)

        def halo_table(e):
            return jnp.where(sub < 4, row(side(e), 1), row(side(e + 1), -1))

        place(halo_table(-1), row_of(-1, 4))
        for e in [0, 1, 2, 19, 20, 21]:
            table = row(side(e), 0)
            for t in range(4):
                place(table, row_of(e, t))
            place(halo_table(e), row_of(e, 4))
        place(halo_table(18), row_of(18, 4))
        edge = halo_table(HALO)

        def middle(e):
            place(edge, pl.multiple_of(row_of(e, 4), 8))

        over_rows(3, 18, 5, middle)

    def image_fields(j):
        return (
            [(u.at[j, c], d) for d in (0, 1) for c in (0, 1)],
            [(u.at[j, 0], 0, 0), (u.at[j, 1], 0, 0)],
        )

    def send_halo(j):
        fields, cells = image_fields(j)
        pack_y(uy_s.at[j], fields)
        pack_corners(uc_s.at[j], cells)
        send_x(fields, EU + 4 * j)
        send_y(uy_s.at[j], uy_r.at[j], EU + 4 * j + 2)
        send_corners(uc_s.at[j], uc_r.at[j], EU + 4 * j + 3)

    def take_halo(j):
        fields, cells = image_fields(j)
        take_x(fields, EU + 4 * j)
        take(uy_r.at[j], sem_r.at[EU + 4 * j + 2])
        take(uc_r.at[j], sem_r.at[EU + 4 * j + 3])
        unpack_y(uy_r.at[j], fields, lambda at: True)
        unpack_corners(uc_r.at[j], cells)

    def over_own(body):
        def row(x):
            for t in range(4):
                body(pl.multiple_of(row_of(x + HALO, t), 8))

        over_rows(0, NXD, 4, row)

    columns = []
    lengths = []

    def finish(j, dots):
        squared = dots[0]
        col = [(dots[1 + 2 * i], dots[2 + 2 * i]) for i in range(j)]
        for re, im in col:
            squared = squared - (re * re + im * im)
        if j > 0:
            squared = jnp.maximum(squared, 0.0)
            columns.append(col)
        lengths.append(jnp.sqrt(squared + epsilon))

    inner(0)
    take_x(soon, E0)
    take(iy_r, sem_r.at[E0 + 2])
    take(ic_r, sem_r.at[E0 + 3])
    unpack_y(iy_r, soon, lambda at: at < 4)
    each_halo(1, lambda e, t: halo_tile(e, t, False, True))

    def halo_first(base):
        here = pl.ds(base, 8)
        put_first(here, z[0, 0, here, :], z[0, 1, here, :])

    over_halo(1, halo_first)
    unpack_y(iy_r, soon, lambda at: at >= 4)
    for k, (dx, dy) in enumerate(CORNERS):
        known = x_inside(-1 if dx < 0 else HALO + NXD) * (y_down if dy < 0 else y_up)
        known = jnp.full((8, 128), known, jnp.int32) > 0
        ic_r[k] = jnp.where(known, ic_r[k], 0.0)
    unpack_corners(ic_r, soon_cells)

    for j in range(ITERS):
        outer(j)
        if j + 1 < ITERS:
            send_halo(j)
        middle_gather(j)
        clear_halo()
        if j == 0:
            take_late()
        if j + 1 < ITERS:
            take_halo(j)
        end_gather(j)
        coarse_solve(j)
        finish(j, all_products(j))
        inverse = 1.0 / lengths[j]
        col = columns[j - 1] if j else []

        def make_basis(base):
            here = pl.ds(base, 8)
            a, b = z[j, 0, here, :], z[j, 1, here, :]
            for i, (re, im) in enumerate(col):
                c, d = v[i, 0, here, :], v[i, 1, here, :]
                a = a - (re * c - im * d)
                b = b - (re * d + im * c)
            v[j, 0, here, :] = a * inverse
            v[j, 1, here, :] = b * inverse

        def make_start(base):
            here = pl.ds(base, 8)
            a, b = u[j, 0, here, :], u[j, 1, here, :]
            for i, (re, im) in enumerate(col):
                c, d = z[i + 1, 0, here, :], z[i + 1, 1, here, :]
                a = a - (re * c - im * d)
                b = b - (re * d + im * c)
            z[j + 1, 0, here, :] = a
            z[j + 1, 1, here, :] = b

        if j + 1 < ITERS:
            over_tiles(2, make_start, 4)
        else:
            over_own(make_start)
        zn = z.at[j + 1]
        last = j + 1 == ITERS

        def make_image(base):
            here = pl.ds(base, 8)
            _, _, w0, w1 = operate(p, base)
            a, b = (zn[0, here, :] + w0) * inverse, (zn[1, here, :] + w1) * inverse
            zn[0, here, :] = a
            zn[1, here, :] = b
            if not last:
                put_first(here, a, b)

        prolong_own(j)
        over_own(make_image)
        over_own(make_basis)
        inner(j + 1)
        prolong_halo(j)
        if not last:
            over_halo(2, make_image)

        def add_edges(e, t, shifts):
            base = row_of(e, t)
            if not isinstance(e, int):
                base = pl.multiple_of(base, 8)
            here = pl.ds(base, 8)
            edge = [zn[0, here, :], zn[1, here, :]]
            for c in range(2):
                for shift in shifts:
                    beyond = p[c, pl.ds(base + shift, 8), :]
                    if shift == 1:
                        beyond = jnp.where(sub == 7, beyond, 0.0)
                    if shift == -1:
                        beyond = jnp.where(sub == 0, beyond, 0.0)
                    edge[c] = edge[c] - beyond * inverse
                zn[c, here, :] = edge[c]
            if not last:
                put_first(here, edge[0], edge[1])

        for e, shift in ((HALO, -PITCH), (HALO + NXD - 1, PITCH)):
            add_edges(e, 0, (shift, -1))
            add_edges(e, 1, (shift,))
            add_edges(e, 2, (shift,))
            add_edges(e, 3, (shift, 1))

        def y_edges(e):
            add_edges(e, 0, (-1,))
            add_edges(e, 3, (1,))

        over_rows(HALO + 1, HALO + NXD - 1, 7, y_edges)

    outer(ITERS)
    middle_gather(ITERS)

    def times(a, b):
        return (a[0] * b[0] - a[1] * b[1], a[0] * b[1] + a[1] * b[0])

    def conj_times(a, b):
        return (a[0] * b[0] + a[1] * b[1], a[0] * b[1] - a[1] * b[0])

    rotations, upper, diagonal = [], [], []
    target = [(lengths[0], zero)]

    def rotate(j):
        col = list(columns[j])
        for k, (c, s) in enumerate(rotations):
            head, tail = col[k], col[k + 1]
            turned = conj_times(c, head)
            other = times(c, tail)
            col[k] = (turned[0] + s * tail[0], turned[1] + s * tail[1])
            col[k + 1] = (other[0] - s * head[0], other[1] - s * head[1])
        below = lengths[j + 1]
        a = col[j]
        size = jnp.sqrt(a[0] * a[0] + a[1] * a[1] + below * below)
        c, s = (a[0] / size, a[1] / size), below / size
        rotations.append((c, s))
        upper.append(col)
        diagonal.append(size)
        last = target[j]
        target[j] = conj_times(c, last)
        target.append((-s * last[0], -s * last[1]))
    for j in range(ITERS - 1):
        rotate(j)
    end_gather(ITERS)
    finish(ITERS, all_products(ITERS))
    rotate(ITERS - 1)
    solved = [None] * ITERS
    for j in reversed(range(ITERS)):
        re, im = target[j]
        for k in range(j + 1, ITERS):
            part = times(upper[k][j], solved[k])
            re, im = re - part[0], im - part[1]
        solved[j] = (re / diagonal[j], im / diagonal[j])

    weights = [None] * ITERS
    for j in reversed(range(ITERS)):
        inverse = 1.0 / lengths[j]
        weights[j] = (solved[j][0] * inverse, solved[j][1] * inverse)
        if j:
            for i, h in enumerate(columns[j - 1]):
                part = times(h, weights[j])
                solved[i] = (solved[i][0] - part[0], solved[i][1] - part[1])

    c_re, c_im = zero, zero
    for j in range(ITERS):
        wr, wi = weights[j]
        row = jnp.broadcast_to(cown[j, 0], (8, 128))
        c_re = c_re + wr * row
        c_im = c_im + wi * row
    turned = jnp.where(lane < 16, -pltpu.roll(c_im, 112, axis=1), pltpu.roll(c_im, 16, axis=1))
    table = jnp.where(lane < 32, c_re + turned, 0.0)

    def write(x):
        for t in range(4):
            here = pl.ds(pl.multiple_of(row_of(x + HALO, t), 8), 8)
            a, b = spread(table, here)
            for j in range(ITERS):
                wr, wi = weights[j]
                c, d = m[j, 0, here, :], m[j, 1, here, :]
                a = a + (wr * c - wi * d)
                b = b + (wr * d + wi * c)
            sol[0, x, pl.ds(8 * t, 8), :] = a
            sol[1, x, pl.ds(8 * t, 8), :] = b

    over_rows(0, NXD, 4, write)

    h_re, h_im = zero, zero
    for j in range(ITERS):
        for i, (re, im) in enumerate(columns[j]):
            spot = (sub == j) & (lane == i)
            h_re = jnp.where(spot, re, h_re)
            h_im = jnp.where(spot, im, h_im)
        h_re = jnp.where((sub == j) & (lane == j + 1), lengths[j + 1], h_re)
    hess[0] = h_re[:ITERS, : ITERS + 1]
    hess[1] = h_im[:ITERS, : ITERS + 1]

    for fields, kind, y_out, c_out in ((soon, E0, iy_s, ic_s), (late, E1, ly_s, lc_s)):
        if kind != E0:
            take_sent_x(fields, kind)
        take(y_out, sem_s.at[kind + 2])
        take(c_out, sem_s.at[kind + 3])
    for j in range(ITERS + 1):
        take(g1.at[j, pl.ds(0, 30)], sem_s.at[S1 + j])
        take(g2.at[j, pl.ds(0, 75)], sem_s.at[S2 + j])
    for j in range(ITERS):
        take(crecv.at[j], sem_s.at[CX + j])
        if j + 1 < ITERS:
            take_sent_x(image_fields(j)[0], EU + 4 * j)
            take(uy_s.at[j], sem_s.at[EU + 4 * j + 2])
            take(uc_s.at[j], sem_s.at[EU + 4 * j + 3])


def body(*args):
    field = pltpu.VMEM((2, ROWS, 128), F32)
    plane = pltpu.VMEM((ROWS, 128), F32)

    def fields(n):
        return pltpu.VMEM((n, 2, ROWS, 128), F32)

    vmem = pl.BlockSpec(memory_space=pltpu.VMEM)
    solution, hessenberg = pl.pallas_call(
        kernel,
        out_shape=(
            pltpu.VMEM(args[0].shape, F32),
            pltpu.VMEM((2, ITERS, ITERS + 1), F32),
        ),
        in_specs=[pl.BlockSpec(memory_space=pl.ANY)] * 5,
        out_specs=(vmem, vmem),
        scratch_shapes=[
            *[pltpu.VMEM(a.shape, a.dtype) for a in args],
            *[plane] * 7,
            pltpu.VMEM((ROWS, 128), jnp.int32),
            fields(5), fields(4), fields(4), fields(4),
            field, field,
            pltpu.VMEM((2, NXD * NYD, 128), F32),
            pltpu.VMEM((48, 8, 128), F32),
            pltpu.VMEM((64, 16, 128), F32),
            pltpu.VMEM((64, 16, 128), F32),
            pltpu.VMEM((5, 32, 1, 128), F32),
            pltpu.VMEM((5, 80, 1, 128), F32),
            pltpu.VMEM((4, 1, 1, 128), F32),
            pltpu.VMEM((4, 8, 1, 128), F32),
            pltpu.VMEM((2, 6, 16, 128), F32),
            pltpu.VMEM((2, 6, 16, 128), F32),
            pltpu.VMEM((4, 8, 128), F32),
            pltpu.VMEM((4, 8, 128), F32),
            pltpu.VMEM((2, 5, 16, 128), F32),
            pltpu.VMEM((2, 5, 16, 128), F32),
            pltpu.VMEM((4, 8, 128), F32),
            pltpu.VMEM((4, 8, 128), F32),
            pltpu.VMEM((3, 2, 4, 16, 128), F32),
            pltpu.VMEM((3, 2, 4, 16, 128), F32),
            pltpu.VMEM((3, 4, 8, 128), F32),
            pltpu.VMEM((3, 4, 8, 128), F32),
            pltpu.SemaphoreType.DMA((34,)),
            pltpu.SemaphoreType.DMA((34,)),
            pltpu.SemaphoreType.DMA((5,)),
        ],
        compiler_params=pltpu.CompilerParams(
            collective_id=0, has_side_effects=True, vmem_limit_bytes=60 * 1024 * 1024
        ),
    )(*args)
    return solution, hessenberg.transpose(0, 2, 1)


def solution(mesh):
    finer = Mesh(mesh.devices.reshape(2, 4, 2, 4, 4), AXES)
    in_specs = (
        P(None, GX, GY, None),
        P(GX, GY, None),
        P(GX, GY, None),
        P(GX, GY, None),
        P(None, GX + GY, None),
    )
    out_specs = (P(None, GX, GY, None), P())
    return jax.shard_map(body, mesh=finer, in_specs=in_specs, out_specs=out_specs, check_vma=False)
```
